32 devices in a mesh: group: 4 (over y, x), dp: 8 (over z, core).
Axes of the slice: x: 2, y: 2, z: 4, core: 2. Of those that a mesh axis runs over, the one named last changes fastest.
Arguments:
- observations: bfloat16 [64, 64, 4096], P('dp', None, 'group'), may hold values from -6 to 6
- next_observations: bfloat16 [1024, 4096], P('dp', 'group'), may hold values from -6 to 6
- trunk_weights: bfloat16 [2, 4096, 4096], P(None, 'dp', 'group'), may hold values from -0.125 to 0.125
- head_weights: bfloat16 [4096, 19], P('group'), may hold values from -0.25 to 0.25
- acting_policy_logits: float32 [64, 63, 18], P('dp'), may hold values from -16 to 330, as said below
- actions: int32 [64, 63], P('dp'), may hold values from 0 to 17
- rewards: float32 [64, 63], P('dp'), may hold values from -6 to 6
- episode_finished: int32 [64, 63], P('dp'), may hold values 0 or 1
Outputs:
- trunk_grads: float32 [2, 4096, 4096], P(None, 'dp', 'group')
- head_grads: float32 [4096, 19], P(('group', 'dp'))
- actor_logits: float32 [1024, 18], P('dp')
The draws below stay inside these ranges and needn't reach their ends.
Inputs may be any that keep to these rules, and one draw needn't show every extreme that they name: `acting_policy_logits`: Real-valued scores, one row for each step and trajectory.
All inputs are finite; a program needn't handle non-finite values. No bound on the sum of `episode_finished` on one device may be relied on, other than what follows from the above.
Results may differ from the reference program's by a relative error of at most 0.012.
Values may be sent and summed in bfloat16 or wider, within the bound.
A program may use at most 128 MiB of HBM per device.

```python
import jax
import jax.numpy as jnp
from jax import lax

D = 4096
A = 18
HEADS = 19
LAYERS = 2
STEPS = 64
TRAJ = 64
ACTORS = 1024


def draw_acting_policy_logits(key, part):
    base_key = jax.random.fold_in(key, 11)
    first_key = jax.random.fold_in(base_key, 0)
    shape = (TRAJ, STEPS - 1, A)
    score_values = jnp.clip(3.0 * jax.random.normal(first_key, shape, jnp.float32), -15.0, 15.0)
    return score_values


def plant(entries, stream_key, low, top_value):
    dims = entries.shape
    spot = [jax.random.randint(jax.random.fold_in(stream_key, axis), (), 0, dims[axis]) for axis in range(len(dims))]
    entries = entries.at[tuple(spot)].set(low)
    longest = dims.index(max(dims))
    spot[longest] = (spot[longest] + 1) % dims[longest]
    return entries.at[tuple(spot)].set(top_value)


def block_scale(stream_key, shape, shards, smallest, top_value):
    level = 1.0
    for axis_at, parts in shards:
        draws = jax.random.uniform(jax.random.fold_in(jax.random.fold_in(stream_key, 6), axis_at), (parts,), jnp.float32, smallest / len(shards), top_value / len(shards))
        level = level * jnp.repeat(jnp.exp(draws), shape[axis_at] // parts).reshape((-1,) + (1,) * (len(shape) - 1 - axis_at))
    return level


def bell_draw(own_key, extent, deviation, limit, cuts=(), kind=jnp.bfloat16):
    array = jax.random.normal(own_key, extent, jnp.float32) * deviation
    if len(cuts) > 0:
        array = block_scale(own_key, extent, cuts, -0.22, 0.18) * array
    return jnp.clip(array, min=-limit, max=limit).astype(kind)


def setup_inputs(seed: int = 0) -> dict:
    key_of = jax.random.split(jax.random.key(seed), 9)
    observations = bell_draw(key_of[0], (TRAJ, STEPS, D), 1.0, 6.0, ((0, 8), (2, 4)))
    next_observations = bell_draw(key_of[1], (ACTORS, D), 1.0, 6.0, ((0, 8), (1, 4)))
    trunk_weights = bell_draw(key_of[2], (LAYERS, D, D), (D // 2) ** -0.5, 0.125, ((1, 8), (2, 4)))
    head_weights = bell_draw(key_of[3], (D, HEADS), (D // 9) ** -0.5, 0.25, ((0, 4),))
    acting_policy_logits = draw_acting_policy_logits(jax.random.fold_in(key_of[8], 71), 0)
    actions = plant(jax.random.randint(key_of[5], (TRAJ, STEPS - 1), 0, A), jax.random.fold_in(key_of[5], 1), 0, A - 1).astype(jnp.int32)
    rewards = bell_draw(key_of[6], (TRAJ, STEPS - 1), 1.0, 6.0, ((0, 8),), jnp.float32)
    episode_finished = plant((jax.random.randint(key_of[7], (TRAJ, STEPS - 1), 0, 16) < 1).astype(jnp.int32), jax.random.fold_in(key_of[7], 1), 0, 1)
    return dict(observations=observations, next_observations=next_observations, trunk_weights=trunk_weights, head_weights=head_weights, acting_policy_logits=acting_policy_logits, actions=actions, rewards=rewards, episode_finished=episode_finished)


discount_rate = 0.99
value_weight = 0.5
entropy_weight = 0.1
loss_divisor = 16.0


def contract_rows(left, right):
    return lax.dot_general(left, right, (((0,), (0,)), ((), ())), preferred_element_type=jnp.float32)


def contract_cols(left, right):
    return lax.dot_general(left, right, (((1,), (1,)), ((), ())), preferred_element_type=jnp.float32)


def silu_slope(pre_value):
    sigma = jax.nn.sigmoid(pre_value)
    return sigma * (1.0 + pre_value * (1.0 - sigma))


def importance_trace_gradients(learner_output, acting_policy_logits, actions, rewards, episode_finished):
    number_of_actions = acting_policy_logits.shape[-1]
    logits = learner_output[:, :, :number_of_actions]
    values = learner_output[:, :, number_of_actions]
    log_policy = jax.nn.log_softmax(logits[:, :-1], axis=-1)
    log_behave = jax.nn.log_softmax(acting_policy_logits, axis=-1)
    chosen = (actions[:, :, None] == jnp.arange(number_of_actions, dtype=jnp.int32)[None, None, :]).astype(jnp.float32)
    ratio = jnp.exp(jnp.sum((log_policy - log_behave) * chosen, axis=-1))
    clipped = jnp.minimum(ratio, 1.0)
    discount = discount_rate * (1.0 - episode_finished.astype(jnp.float32))
    current = values[:, :-1]
    following = values[:, 1:]
    deltas = clipped * (rewards + discount * following - current)

    def backward_step(carried, step_item):
        delta_now, factor_now = step_item
        carried = delta_now + factor_now * carried
        return carried, carried

    start_carry = jnp.zeros((values.shape[0],), jnp.float32)
    _, corrections = lax.scan(backward_step, start_carry, (deltas.T, (discount * clipped).T), reverse=True)
    targets = current + corrections.T
    next_targets = jnp.concatenate([targets[:, 1:], values[:, -1:]], axis=1)
    advantage = clipped * (rewards + discount * next_targets - current)
    probability = jnp.exp(log_policy)
    entropy = -jnp.sum(probability * log_policy, axis=-1)
    logit_grad = (-advantage[..., None] * (chosen - probability)
                  + entropy_weight * probability * (log_policy + entropy[..., None])) / loss_divisor
    value_grad = -value_weight * (targets - current) / loss_divisor
    step_grad = jnp.concatenate([logit_grad, value_grad[..., None]], axis=-1)
    last_row = jnp.zeros((values.shape[0], 1, number_of_actions + 1), jnp.float32)
    return jnp.concatenate([step_grad, last_row], axis=1)


def reference(observations, next_observations, trunk_weights, head_weights, acting_policy_logits, actions, rewards, episode_finished):
    traj_total, step_total, width = observations.shape
    learner_rows = traj_total * step_total
    number_of_actions = acting_policy_logits.shape[-1]
    layer_input = jnp.concatenate([observations.reshape(learner_rows, width), next_observations], axis=0)
    inputs_kept = []
    products_kept = []
    for layer_index in range(trunk_weights.shape[0]):
        inputs_kept.append(layer_input[:learner_rows])
        product = jnp.dot(layer_input, trunk_weights[layer_index], preferred_element_type=jnp.float32)
        products_kept.append(product[:learner_rows])
        layer_input = jax.nn.silu(product).astype(jnp.bfloat16)
    head_out = jnp.dot(layer_input, head_weights, preferred_element_type=jnp.float32)
    actor_logits = head_out[learner_rows:, :number_of_actions]
    learner_output = head_out[:learner_rows].reshape(traj_total, step_total, number_of_actions + 1)
    output_gradient = importance_trace_gradients(learner_output, acting_policy_logits, actions, rewards, episode_finished)
    output_gradient = output_gradient.reshape(learner_rows, number_of_actions + 1).astype(jnp.bfloat16)
    head_grads = contract_rows(layer_input[:learner_rows], output_gradient)
    input_grad = contract_cols(output_gradient, head_weights)
    layer_total = trunk_weights.shape[0]
    grad_list = [None] * layer_total
    for layer_index in range(layer_total - 1, -1, -1):
        pre_grad = (input_grad * silu_slope(products_kept[layer_index])).astype(jnp.bfloat16)
        grad_list[layer_index] = contract_rows(inputs_kept[layer_index], pre_grad)
        if layer_index > 0:
            input_grad = contract_cols(pre_grad, trunk_weights[layer_index])
    return jnp.stack(grad_list), head_grads, actor_logits
```

```python
import functools

import jax
import jax.numpy as jnp
from jax import lax
from jax.experimental import pallas as pl
from jax.experimental.pallas import tpu as pltpu
from jax.sharding import PartitionSpec as P

discount_rate = 0.99
value_weight = 0.5
entropy_weight = 0.1
loss_divisor = 16.0


def contract_rows(left, right):
    return lax.dot_general(
        left, right, (((0,), (0,)), ((), ())), preferred_element_type=jnp.float32
    )


def contract_cols(left, right):
    return lax.dot_general(
        left, right, (((1,), (1,)), ((), ())), preferred_element_type=jnp.float32
    )


def silu_slope(pre_value):
    sigma = jax.nn.sigmoid(pre_value)
    return sigma * (1.0 + pre_value * (1.0 - sigma))


def importance_trace_gradients(
    learner_output, acting_policy_logits, actions, rewards, episode_finished
):
    log_behave = jax.nn.log_softmax(acting_policy_logits, axis=-1)
    chosen = actions[:, :, None] == jnp.arange(log_behave.shape[-1], dtype=jnp.int32)
    behave = jnp.sum(jnp.where(chosen, log_behave, 0.0), axis=-1)
    return trace_gradients(
        learner_output, behave, actions, rewards, episode_finished.astype(jnp.float32)
    )


def trace_gradients_packed(learner_output, packed):
    behave, actions, rewards, finished = packed
    return trace_gradients(learner_output, behave, actions.astype(jnp.int32), rewards, finished)


def trace_gradients(learner_output, behave, actions, rewards, finished):
    number_of_actions = learner_output.shape[-1] - 1
    logits = learner_output[:, :, :number_of_actions]
    values = learner_output[:, :, number_of_actions]
    log_policy = jax.nn.log_softmax(logits[:, :-1], axis=-1)
    chosen = (
        actions[:, :, None] == jnp.arange(number_of_actions, dtype=jnp.int32)[None, None, :]
    ).astype(jnp.float32)
    ratio = jnp.exp(jnp.sum(log_policy * chosen, axis=-1) - behave)
    clipped = jnp.minimum(ratio, 1.0)
    discount = discount_rate * (1.0 - finished)
    current = values[:, :-1]
    following = values[:, 1:]
    deltas = clipped * (rewards + discount * following - current)

    corrections, factors = deltas, discount * clipped
    reach, span = 1, deltas.shape[1]
    while reach < span:
        later = jnp.pad(corrections[:, reach:], ((0, 0), (0, reach)))
        later_factors = jnp.pad(factors[:, reach:], ((0, 0), (0, reach)))
        corrections = corrections + factors * later
        factors = factors * later_factors
        reach *= 2
    targets = current + corrections
    next_targets = jnp.concatenate([targets[:, 1:], values[:, -1:]], axis=1)
    advantage = clipped * (rewards + discount * next_targets - current)
    probability = jnp.exp(log_policy)
    entropy = -jnp.sum(probability * log_policy, axis=-1)
    logit_grad = (
        -advantage[..., None] * (chosen - probability)
        + entropy_weight * probability * (log_policy + entropy[..., None])
    ) / loss_divisor
    value_grad = -value_weight * (targets - current) / loss_divisor
    step_grad = jnp.concatenate([logit_grad, value_grad[..., None]], axis=-1)
    last_row = jnp.zeros((values.shape[0], 1, number_of_actions + 1), jnp.float32)
    return jnp.concatenate([step_grad, last_row], axis=1)


def swap(block, mask, size):
    return lax.ppermute(block, "group", [(index, index ^ mask) for index in range(size)])


def gather_features(block, size):
    if size != 4:
        return lax.all_gather(block, "group", axis=1, tiled=True)
    me = lax.axis_index("group")
    rows, width = block.shape
    half = rows // 2
    from_near = swap(block, 1, size)
    from_far = swap(block, 2, size)
    top = swap(from_near[:half], 2, size)
    bottom = swap(from_far[half:], 1, size)
    whole = jnp.zeros((rows, size * width), block.dtype)
    whole = lax.dynamic_update_slice(whole, block, (0, me * width))
    whole = lax.dynamic_update_slice(whole, from_near, (0, (me ^ 1) * width))
    whole = lax.dynamic_update_slice(whole, from_far, (0, (me ^ 2) * width))
    whole = lax.dynamic_update_slice(whole, top, (0, (me ^ 3) * width))
    return lax.dynamic_update_slice(whole, bottom, (half, (me ^ 3) * width))


def scatter_features(partial, size):
    if size != 4:
        return lax.psum_scatter(partial, "group", scatter_dimension=1, tiled=True)
    me = lax.axis_index("group")
    rows, width = partial.shape[0], partial.shape[1] // size
    half = rows // 2
    wire = jnp.bfloat16

    def part(start, mask):
        piece = lax.dynamic_slice(partial, (start, (me ^ mask) * width), (half, width))
        return piece

    def reduce_half(start, first, second):
        theirs = jnp.concatenate([part(start, first), part(start, 3)], axis=0)
        got = swap(theirs, first, size)
        onward = part(start, second).astype(jnp.float32) + got[half:].astype(jnp.float32)
        mine = part(start, 0).astype(jnp.float32) + got[:half].astype(jnp.float32)
        return mine + swap(onward.astype(wire), second, size).astype(jnp.float32)

    return jnp.concatenate([reduce_half(0, 1, 2), reduce_half(half, 2, 1)], axis=0)


def scatter_rows(block, size):
    if size & (size - 1):
        return lax.psum_scatter(block, "dp", scatter_dimension=0, tiled=True)
    me = lax.axis_index("dp")
    mask = size // 2
    while mask:
        half = block.shape[0] // 2
        upper = (me & mask) > 0
        theirs = jnp.where(upper, block[:half], block[half:])
        mine = jnp.where(upper, block[half:], block[:half])
        block = mine + lax.ppermute(theirs, "dp", [(i, i ^ mask) for i in range(size)])
        mask //= 2
    return block


def swap_cores(block, size):
    return lax.ppermute(block, "dp", [(index, index ^ 1) for index in range(size)])


def split_for_pair(whole, size):
    core = lax.axis_index("dp") % 2
    rows, width = whole.shape
    by_owner = whole.reshape(rows, size // 2, 2, width // size)

    def features_of(owner):
        picked = lax.dynamic_slice_in_dim(by_owner, owner, 1, axis=2)
        return picked.reshape(rows, width // 2)

    return features_of(core), swap_cores(features_of(1 - core), size)


def sum_group(block, size):
    if size != 4:
        return lax.psum(block, "group")
    block = block + swap(block, 1, size)
    return block + swap(block, 2, size)


def per_device(
    group_size,
    dp_size,
    observations,
    next_observations,
    trunk_weights,
    head_weights,
    acting_policy_logits,
    actions,
    rewards,
    episode_finished,
):
    traj_count, step_count, feature_block = observations.shape
    learner_rows = traj_count * step_count
    number_of_actions = acting_policy_logits.shape[-1]
    layer_total = trunk_weights.shape[0]
    own_rows = observations.reshape(learner_rows, feature_block)
    gathered_weights = [
        lax.all_gather(trunk_weights[layer_index], "dp", axis=0, tiled=True)
        for layer_index in range(layer_total)
    ]
    current = jnp.concatenate([own_rows, next_observations], axis=0)
    pair_inputs = []
    products_block = []
    for layer_index in range(layer_total):
        whole = gather_features(current, group_size)
        product = jnp.dot(
            whole, gathered_weights[layer_index], preferred_element_type=jnp.float32
        )
        pair_inputs.append(split_for_pair(whole[:learner_rows], dp_size))
        products_block.append(product[:learner_rows])
        current = jax.nn.silu(product).astype(jnp.bfloat16)
    partial_head = jnp.dot(current, head_weights, preferred_element_type=jnp.float32)
    totals = sum_group(partial_head, group_size)
    last_block = current[:learner_rows]
    head_out = totals[:learner_rows]
    actor_logits = totals[learner_rows:, :number_of_actions]
    learner_output = head_out.reshape(traj_count, step_count, number_of_actions + 1)
    output_gradient = importance_trace_gradients(
        learner_output, acting_policy_logits, actions, rewards, episode_finished
    )
    output_gradient = output_gradient.reshape(learner_rows, number_of_actions + 1).astype(
        jnp.bfloat16
    )
    input_grad = contract_cols(output_gradient, head_weights)
    grad_list = [None] * layer_total
    for layer_index in range(layer_total - 1, -1, -1):
        pre_grad = (input_grad * silu_slope(products_block[layer_index])).astype(jnp.bfloat16)
        near_inputs, far_inputs = pair_inputs[layer_index]
        far_grad = swap_cores(pre_grad, dp_size)
        partial = contract_rows(near_inputs, pre_grad) + contract_rows(far_inputs, far_grad)
        partial = partial.astype(jnp.bfloat16)
        partial, pre_grad = lax.optimization_barrier((partial, pre_grad))
        grad_list[layer_index] = lax.psum_scatter(
            partial,
            "dp",
            scatter_dimension=0,
            tiled=True,
            axis_index_groups=[list(range(core, dp_size, 2)) for core in range(2)],
        ).astype(jnp.float32)
        if layer_index > 0:
            full_grad = contract_cols(pre_grad, gathered_weights[layer_index]).astype(jnp.bfloat16)
            input_grad = scatter_features(full_grad, group_size)
    head_partial = contract_rows(last_block, output_gradient)
    head_grads = scatter_rows(head_partial, dp_size)
    return (jnp.stack(grad_list), head_grads, actor_logits)


MESH = pl.DeviceIdType.MESH
PIECES = 2
TILE = 256
PRODUCT_TILE = 512


class Place:
    def __init__(self):
        group, dp = lax.axis_index("group"), lax.axis_index("dp")
        self.group, self.dp = group, dp
        self.x, self.core, self.z = group % 2, dp % 2, dp // 2
        self.near_x = group + 1 - 2 * self.x
        self.near_y = (group + 2) % 4
        self.planes = lax.axis_size("dp") // 2
        self.to_x = (self.near_x, dp)
        self.to_y = (self.near_y, dp)
        self.to_core = (group, dp + 1 - 2 * self.core)
        self.to_way = ((group, dp + 2), (group, dp - 2))

    def source(self, way, far):
        return self.z - far if way == 0 else self.z + far

    def has_source(self, way, far):
        return self.z >= far if way == 0 else self.z + far < self.planes

    def has_next(self, way):
        return self.z + 1 < self.planes if way == 0 else self.z > 0

    def greet(self):
        barrier = pltpu.get_barrier_semaphore()
        for peer in (self.to_x, self.to_y, self.to_core):
            pl.semaphore_signal(barrier, inc=1, device_id=peer, device_id_type=MESH)
        for way in range(2):
            @pl.when(self.has_next(way))
            def _():
                pl.semaphore_signal(
                    barrier, inc=1, device_id=self.to_way[way], device_id_type=MESH)
        inner = jnp.logical_and(self.has_next(0), self.has_next(1))
        pl.semaphore_wait(barrier, jnp.where(inner, 5, 4))


def remote(source, target, sent, landed, peer):
    return pltpu.make_async_remote_copy(
        src_ref=source, dst_ref=target, send_sem=sent, recv_sem=landed,
        device_id=peer, device_id_type=MESH)


def forward_kernel(
    observations, next_observations, weights,
    pre_out, inputs_out, weights_out, last_out,
    weight_buf, input_buf, total, local_sem, x_sent, x_landed, z_sent, z_landed,
    c_sent, c_landed, out_sem,
):
    place = Place()
    group, dp, z, core = place.group, place.dp, place.z, place.core
    layers, in_block, width = weights.shape
    learner_rows = observations.shape[0]
    rows = learner_rows + next_observations.shape[0]
    half = rows // 2
    piece_rows = in_block // PIECES
    halves = (pl.ds(0, half), pl.ds(half, half))

    loads = [
        pltpu.make_async_copy(
            observations, input_buf.at[0, group, pl.ds(0, learner_rows)], local_sem.at[0]),
        pltpu.make_async_copy(
            next_observations,
            input_buf.at[0, group, pl.ds(learner_rows, rows - learner_rows)], local_sem.at[1]),
    ] + [
        pltpu.make_async_copy(weights.at[layer], weight_buf.at[layer, dp], local_sem.at[2 + layer])
        for layer in range(layers)
    ]
    for load in loads:
        load.start()
    place.greet()

    def weight_copy(layer, way, far, piece):
        block = 2 * place.source(way, far) + core
        span = weight_buf.at[layer, block, pl.ds(piece * piece_rows, piece_rows)]
        source = weights.at[layer, pl.ds(piece * piece_rows, piece_rows)] if far == 0 else span
        return remote(source, span, z_sent.at[layer, way, far, piece],
                      z_landed.at[layer, way, far, piece], place.to_way[way])

    def weight_arrival(layer, way, far, piece):
        block = 2 * place.source(way, far) + core
        span = weight_buf.at[layer, block, pl.ds(piece * piece_rows, piece_rows)]
        return remote(span, span, z_sent.at[layer, way, far - 1, piece],
                      z_landed.at[layer, way, far - 1, piece], place.to_core)

    def core_copy(layer, way, far, piece, arriving=False):
        owner = 1 - core if arriving else core
        block = 2 * place.source(way, far) + owner
        span = weight_buf.at[layer, block, pl.ds(piece * piece_rows, piece_rows)]
        source = span
        if far == 0 and not arriving:
            source = weights.at[layer, pl.ds(piece * piece_rows, piece_rows)]
        return remote(source, span, c_sent.at[layer, way, far, piece],
                      c_landed.at[layer, way, far, piece], place.to_core)

    def send_own_weights(layer, way):
        for piece in range(PIECES):
            weight_copy(layer, way, 0, piece).start()

    def send_own_core(layer):
        for piece in range(PIECES):
            core_copy(layer, 0, 0, piece).start()

    def own_turn(far):
        for way in range(2):
            edge = z == far if way == 0 else place.planes - 1 - z == far
            @pl.when(jnp.logical_and(edge, place.has_next(way)))
            def _():
                for layer in range(1, layers):
                    send_own_weights(layer, way)

    def relay(layer, far, piece):
        for way in range(2):
            @pl.when(place.has_source(way, far))
            def _():
                weight_arrival(layer, way, far, piece).wait_recv()
                @pl.when(place.has_next(way))
                def _():
                    weight_copy(layer, way, far, piece).start()
                core_copy(layer, way, far, piece).start()

    def input_copy(layer, stage, kind, arriving=False):
        lane, part = kind
        peer = (place.to_x, place.to_y)[lane]
        if stage == 0:
            quarter = (place.near_x, place.near_y)[lane] if arriving else group
        else:
            other = (place.near_y, place.near_x)[lane]
            quarter = (place.near_x + 2) % 4 if arriving else other
        span = input_buf.at[layer, quarter, halves[part]]
        index = (layer, stage, lane, part)
        return remote(span, span, x_sent.at[index], x_landed.at[index], peer)

    FIRST = ((0, 0), (1, 1))
    SECOND = ((0, 1), (1, 0))
    ONWARD = ((1, 0), (0, 1))

    def multiply(layer, plane):
        left = input_buf.at[layer, plane]
        right = weight_buf.at[layer, pl.ds(2 * plane, 2)]

        def step(tile, carry):
            columns = pl.ds(pl.multiple_of(tile * TILE, TILE), TILE)
            total[layer, :, columns] += jnp.dot(
                left[...], right[:, :, columns].reshape(width, TILE),
                preferred_element_type=jnp.float32)
            return carry
        lax.fori_loop(0, width // TILE, step, 0)

    def core_arrivals(layer, far):
        for way in range(2 if far else 1):
            def wait():
                for piece in range(PIECES):
                    core_copy(layer, way, far, piece, arriving=True).wait_recv()
            if far:
                pl.when(place.has_source(way, far))(wait)
            else:
                wait()

    def multiply_far(layer, far):
        core_arrivals(layer, far)
        if far == 0:
            multiply(layer, z)
            return
        for way in range(2):
            @pl.when(place.has_source(way, far))
            def _():
                multiply(layer, place.source(way, far))

    def finish(layer, part):
        span = halves[part]
        value = total[layer, span, :]
        result = (value * jax.nn.sigmoid(value)).astype(jnp.bfloat16)
        if layer + 1 < layers:
            input_buf[layer + 1, group, span, :] = result
        else:
            input_buf[layer + 1, 0, span, :] = result

    loads[0].wait()
    loads[1].wait()
    for kind in FIRST + SECOND:
        input_copy(0, 0, kind).start()
    for way in range(2):
        pl.when(place.has_next(way))(functools.partial(send_own_weights, 0, way))
    own_turn(0)
    send_own_core(0)
    total[...] = jnp.zeros_like(total)
    outs = []
    for layer in range(layers):
        relay(layer, 1, 0)
        for kind in FIRST:
            input_copy(layer, 0, kind, True).wait_recv()
        for kind in ONWARD:
            input_copy(layer, 1, kind).start()
        for piece in range(1, PIECES):
            relay(layer, 1, piece)
        if layer == 0:
            own_turn(1)
        for kind in SECOND:
            input_copy(layer, 0, kind, True).wait_recv()
        relay(layer, 2, 0)
        for kind in ONWARD:
            input_copy(layer, 1, kind, True).wait_recv()
        if layer == 0:
            for load in loads[2:]:
                load.wait()
        multiply_far(layer, 0)
        for piece in range(1, PIECES):
            relay(layer, 2, piece)
        if layer == 0:
            own_turn(2)
            send_own_core(1)
        multiply_far(layer, 1)
        for piece in range(PIECES):
            relay(layer, 3, piece)
        multiply_far(layer, 2)
        multiply_far(layer, 3)
        for part in (0, 1):
            finish(layer, part)
            if layer + 1 < layers:
                for kind in FIRST + SECOND:
                    if kind[1] == part:
                        input_copy(layer + 1, 0, kind).start()
        outs.append(pltpu.make_async_copy(
            total.at[layer, pl.ds(0, learner_rows)], pre_out.at[layer], out_sem.at[2 * layer]))
        outs.append(pltpu.make_async_copy(
            input_buf.at[layer, :, pl.ds(0, learner_rows)],
            inputs_out.at[layer], out_sem.at[2 * layer + 1]))
        for out in outs[-2:]:
            out.start()
    finals = [
        pltpu.make_async_copy(input_buf.at[layers, 0], last_out, out_sem.at[2 * layers]),
        pltpu.make_async_copy(weight_buf.at[layers - 1], weights_out, out_sem.at[2 * layers + 1]),
    ]
    for final in finals:
        final.start()
    for layer in range(layers):
        for kind in FIRST + SECOND:
            input_copy(layer, 0, kind).wait_send()
        for kind in ONWARD:
            input_copy(layer, 1, kind).wait_send()
        for piece in range(PIECES):
            core_copy(layer, 0, 0, piece).wait_send()
            for way in range(2):
                pl.when(place.has_next(way))(weight_copy(layer, way, 0, piece).wait_send)
                for far in (1, 2, 3):
                    @pl.when(place.has_source(way, far))
                    def _():
                        pl.when(place.has_next(way))(
                            weight_copy(layer, way, far, piece).wait_send)
                        core_copy(layer, way, far, piece).wait_send()
    for final in outs + finals:
        final.wait()


def forward(observations, next_observations, weights):
    layers, in_block, width = weights.shape
    learner_rows = observations.shape[0]
    rows = learner_rows + next_observations.shape[0]
    bf16, f32 = jnp.bfloat16, jnp.float32
    dma = pltpu.SemaphoreType.DMA
    hbm = pl.BlockSpec(memory_space=pltpu.HBM)
    return pl.pallas_call(
        forward_kernel,
        out_shape=(
            jax.ShapeDtypeStruct((layers, learner_rows, width), f32),
            jax.ShapeDtypeStruct((layers, 4, learner_rows, width), bf16),
            jax.ShapeDtypeStruct((8, in_block, width), bf16),
            jax.ShapeDtypeStruct((rows, width), bf16),
        ),
        in_specs=[hbm] * 3,
        out_specs=(hbm,) * 4,
        scratch_shapes=[
            pltpu.VMEM((layers, 8, in_block, width), bf16),
            pltpu.VMEM((layers + 1, 4, rows, width), bf16),
            pltpu.VMEM((layers, rows, width), f32),
            dma((2 + layers,)),
            dma((layers, 2, 2, 2)), dma((layers, 2, 2, 2)),
            dma((layers, 2, 4, PIECES)), dma((layers, 2, 4, PIECES)),
            dma((layers, 2, 4, PIECES)), dma((layers, 2, 4, PIECES)),
            dma((2 * layers + 2,)),
        ],
        compiler_params=pltpu.CompilerParams(
            collective_id=0, has_side_effects=True, vmem_limit_bytes=60 * 2**20),
        name="forward_trunk",
    )(observations, next_observations, weights)


def backward_kernel(
    top_grad, inputs, pre, weights, grads_out,
    pair_in, pair_grad, weight_buf, pre_buf, line, keep, first_out, first_in,
    second_out, second_in, result, load_sem, c_sent, c_landed, z_sent, z_landed,
    x_sent, x_landed, out_sem,
):
    place = Place()
    group, dp, z, core = place.group, place.dp, place.z, place.core
    planes = place.planes
    layers, quarters, rows, width = inputs.shape
    in_block = width // 2
    half = rows // 2
    piece_rows = in_block // PIECES
    bf16, f32 = jnp.bfloat16, jnp.float32
    own_rows = pl.ds(pl.multiple_of(core * rows, rows), rows)
    other_rows = pl.ds(pl.multiple_of((1 - core) * rows, rows), rows)
    own_cols = pl.ds(pl.multiple_of(core * in_block, in_block), in_block)
    other_cols = pl.ds(pl.multiple_of((1 - core) * in_block, in_block), in_block)
    top = layers - 1

    loads = [pltpu.make_async_copy(top_grad, pair_grad.at[top, own_rows], load_sem.at[0])]
    loads.append(pltpu.make_async_copy(weights, weight_buf, load_sem.at[1]))
    loads += [
        pltpu.make_async_copy(
            inputs.at[layer, :, :, own_cols], pair_in.at[layer, :, own_rows],
            load_sem.at[2 + layer])
        for layer in range(layers)
    ]
    loads.append(pltpu.make_async_copy(pre.at[0], pre_buf, load_sem.at[2 + layers]))
    for index in (0, 1, 2 + top, 2, 2 + layers):
        loads[index].start()
    place.greet()

    def pair_inputs(layer, arriving=False):
        source = inputs.at[layer, :, :, other_cols]
        target = pair_in.at[layer, :, other_rows if arriving else own_rows]
        return remote(source, target, c_sent.at[0, layer], c_landed.at[0, layer], place.to_core)

    def pair_grads(layer, arriving=False):
        target = pair_grad.at[layer, other_rows if arriving else own_rows]
        source = top_grad if layer == top else target
        return remote(source, target, c_sent.at[1, layer], c_landed.at[1, layer], place.to_core)

    pair_grads(top).start()
    for layer in range(top, -1, -1):
        pair_inputs(layer).start()

    halves = (pl.ds(0, half), pl.ds(half, half))
    lanes = ((place.to_x, place.to_y), (place.to_y, place.to_x))
    near = ((place.near_x, place.near_y), (place.near_y, place.near_x))
    far_quarter = (place.near_x + 2) % 4

    def first_copy(part, slot):
        index = (part, slot)
        return remote(first_out.at[index], first_in.at[index], x_sent.at[0, part, slot],
                      x_landed.at[0, part, slot], lanes[part][0])

    def second_copy(part):
        return remote(second_out.at[part], second_in.at[part], x_sent.at[1, part, 0],
                      x_landed.at[1, part, 0], lanes[part][1])

    def input_quarter(quarter, rows_of):
        parts = []
        for block in range(2):
            parts.append(lax.dot_general(
                pair_grad[top, rows_of, :], weight_buf[2 * quarter + block],
                (((1,), (1,)), ((), ())), preferred_element_type=f32))
        return parts

    cores = pl.multiple_of(core * rows, rows)

    def rows_at(part):
        return pl.ds(pl.multiple_of(cores + part * half, half), half)

    def block_cols(block):
        return pl.ds(block * in_block, in_block)

    def send_first(part, slot, quarter):
        for block, value in enumerate(input_quarter(quarter, rows_at(part))):
            first_out[part, slot, :, block_cols(block)] = value.astype(bf16)
        first_copy(part, slot).start()

    def keep_quarter(part, slot, quarter):
        for block, value in enumerate(input_quarter(quarter, rows_at(part))):
            keep[part, slot, :, block_cols(block)] = value

    def order(step):
        table = []
        for at in range(planes):
            up = list(range(planes - 1, at, -1))
            down = list(range(0, at))
            mixed = []
            while up or down:
                if up:
                    mixed.append(up.pop(0))
                if down:
                    mixed.append(down.pop(0))
            table.append((mixed + [at])[step])
        plane = table[-1]
        for at in range(planes - 1):
            plane = jnp.where(z == at, table[at], plane)
        return plane

    def line_send(layer, plane, piece, way):
        source = line.at[layer, plane, pl.ds(piece * piece_rows, piece_rows)]
        if way == 0:
            slot = plane
        else:
            slot = jnp.where(plane == z - 1, planes, plane)
        target = line.at[layer, slot, pl.ds(piece * piece_rows, piece_rows)]
        return remote(source, target, z_sent.at[layer, plane, piece],
                      z_landed.at[layer, slot, piece], place.to_way[way])

    def line_arrival(layer, slot, piece):
        span = line.at[layer, slot, pl.ds(piece * piece_rows, piece_rows)]
        return remote(span, span, z_sent.at[layer, 0, piece],
                      z_landed.at[layer, slot, piece], place.to_core)

    def product(layer, plane, piece, columns):
        left = pair_in[layer, plane, :, pl.ds(piece * piece_rows, piece_rows)]
        return lax.dot_general(
            left, pair_grad[layer, :, columns], (((0,), (0,)), ((), ())),
            preferred_element_type=f32)

    tile = PRODUCT_TILE
    tiles = width // tile

    def over_tiles(body):
        def step(index, carry):
            body(pl.ds(pl.multiple_of(index * tile, tile), tile))
            return carry
        lax.fori_loop(0, tiles, step, 0)

    def pass_on(layer, step):
        plane = order(step)
        upward = plane > z
        fed = jnp.where(upward, z > 0, z + 1 < planes)
        for piece in range(PIECES):
            span = pl.ds(piece * piece_rows, piece_rows)

            @pl.when(fed)
            def _():
                line_arrival(layer, plane, piece).wait_recv()

                def body(columns):
                    value = product(layer, plane, piece, columns)
                    value = value + line[layer, plane, span, columns].astype(f32)
                    line[layer, plane, span, columns] = value.astype(bf16)
                over_tiles(body)

            @pl.when(jnp.logical_not(fed))
            def _():
                def body(columns):
                    value = product(layer, plane, piece, columns)
                    line[layer, plane, span, columns] = value.astype(bf16)
                over_tiles(body)

            pl.when(upward)(line_send(layer, plane, piece, 0).start)
            pl.when(jnp.logical_not(upward))(line_send(layer, plane, piece, 1).start)

    def drain(layer, step):
        plane = order(step)
        for piece in range(PIECES):
            span = line.at[layer, plane, pl.ds(piece * piece_rows, piece_rows)]
            remote(span, span, z_sent.at[layer, plane, piece],
                   z_landed.at[layer, plane, piece], place.to_core).wait_send()

    def own_product(layer):
        for piece in range(PIECES):
            span = pl.ds(piece * piece_rows, piece_rows)

            def body(columns):
                result[layer, span, columns] = product(layer, z, piece, columns)
            over_tiles(body)

    def own_add(layer):
        for piece in range(PIECES):
            span = pl.ds(piece * piece_rows, piece_rows)
            for slot, present in ((z, z > 0), (planes, z + 1 < planes)):
                @pl.when(present)
                def _():
                    line_arrival(layer, slot, piece).wait_recv()
                    result[layer, span, :] += line[layer, slot, span, :].astype(f32)
            pltpu.make_async_copy(
                result.at[layer, span], grads_out.at[layer, span],
                out_sem.at[layer, piece]).start()

    loads[0].wait()
    loads[1].wait()
    for part in range(2):
        send_first(part, 0, far_quarter)
    for part in range(2):
        send_first(part, 1, near[part][0])
    loads[2 + top].wait()
    pair_grads(top, True).wait_recv()
    pair_inputs(top, True).wait_recv()
    pass_on(top, 0)
    for part in range(2):
        keep_quarter(part, 1, near[part][1])
        keep_quarter(part, 0, group)
    for part in range(2):
        first_copy(part, 0).wait_recv()
        second_out[part] = (keep[part, 1] + first_in[part, 0].astype(f32)).astype(bf16)
        second_copy(part).start()
    pass_on(top, 1)
    loads[2 + layers].wait()
    for part in range(2):
        first_copy(part, 1).wait_recv()
        second_copy(part).wait_recv()
        total = keep[part, 0] + first_in[part, 1].astype(f32) + second_in[part].astype(f32)
        value = pre_buf[halves[part], :]
        sigma = jax.nn.sigmoid(value)
        slope = sigma * (1.0 + value * (1.0 - sigma))
        pair_grad[0, rows_at(part), :] = (total * slope).astype(bf16)
    pair_grads(0).start()
    pass_on(top, 2)
    own_product(top)
    loads[2].wait()
    pair_grads(0, True).wait_recv()
    pair_inputs(0, True).wait_recv()
    pass_on(0, 0)
    own_add(top)
    pass_on(0, 1)
    own_product(0)
    pass_on(0, 2)
    own_add(0)

    for layer in range(layers):
        pair_inputs(layer).wait_send()
        pair_grads(layer).wait_send()
        for step in range(planes - 1):
            drain(layer, step)
        for piece in range(PIECES):
            span = pl.ds(piece * piece_rows, piece_rows)
            pltpu.make_async_copy(
                result.at[layer, span], grads_out.at[layer, span],
                out_sem.at[layer, piece]).wait()
    for part in range(2):
        for slot in range(2):
            first_copy(part, slot).wait_send()
        second_copy(part).wait_send()


def backward(top_grad, inputs, pre, weights):
    layers, quarters, rows, width = inputs.shape
    in_block = width // 2
    half = rows // 2
    planes = lax.axis_size("dp") // 2
    bf16, f32 = jnp.bfloat16, jnp.float32
    dma = pltpu.SemaphoreType.DMA
    hbm = pl.BlockSpec(memory_space=pltpu.HBM)
    return pl.pallas_call(
        backward_kernel,
        out_shape=jax.ShapeDtypeStruct((layers, in_block, width), f32),
        in_specs=[hbm] * 4,
        out_specs=hbm,
        scratch_shapes=[
            pltpu.VMEM((layers, quarters, 2 * rows, in_block), bf16),
            pltpu.VMEM((layers, 2 * rows, width), bf16),
            pltpu.VMEM(weights.shape, bf16),
            pltpu.VMEM((rows, width), f32),
            pltpu.VMEM((layers, planes + 1, in_block, width), bf16),
            pltpu.VMEM((2, 2, half, width), f32),
            pltpu.VMEM((2, 2, half, width), bf16),
            pltpu.VMEM((2, 2, half, width), bf16),
            pltpu.VMEM((2, half, width), bf16),
            pltpu.VMEM((2, half, width), bf16),
            pltpu.VMEM((layers, in_block, width), f32),
            dma((3 + layers,)),
            dma((2, layers)), dma((2, layers)),
            dma((layers, planes + 1, PIECES)), dma((layers, planes + 1, PIECES)),
            dma((2, 2, 2)), dma((2, 2, 2)),
            dma((layers, PIECES)),
        ],
        compiler_params=pltpu.CompilerParams(
            collective_id=1, has_side_effects=True, vmem_limit_bytes=60 * 2**20),
        name="backward_trunk",
    )(top_grad, inputs, pre, weights)


def per_device_line(
    group_size, dp_size,
    observations, next_observations, trunk_weights, head_weights,
    acting_policy_logits, actions, rewards, episode_finished,
):
    traj_count, step_count, feature_block = observations.shape
    learner_rows = traj_count * step_count
    number_of_actions = acting_policy_logits.shape[-1]
    layer_total = trunk_weights.shape[0]
    pres, inputs, last_weights, current = forward(
        observations.reshape(learner_rows, feature_block), next_observations, trunk_weights)
    partial_head = jnp.dot(current, head_weights, preferred_element_type=jnp.float32)
    totals = sum_group(partial_head, group_size)
    last_block = current[:learner_rows]
    head_out = totals[:learner_rows]
    actor_logits = totals[learner_rows:, :number_of_actions]
    learner_output = head_out.reshape(traj_count, step_count, number_of_actions + 1)
    output_gradient = importance_trace_gradients(
        learner_output, acting_policy_logits, actions, rewards, episode_finished
    )
    output_gradient = output_gradient.reshape(learner_rows, number_of_actions + 1).astype(
        jnp.bfloat16
    )
    input_grad = contract_cols(output_gradient, head_weights)
    top_grad = (input_grad * silu_slope(pres[-1])).astype(jnp.bfloat16)
    trunk_grads = backward(top_grad, inputs, pres, last_weights)
    head_partial = contract_rows(last_block, output_gradient)
    head_grads = scatter_rows(head_partial, dp_size)
    return (trunk_grads, head_grads, actor_logits)


def solution(mesh):
    in_specs = (
        P("dp", None, "group"),
        P("dp", "group"),
        P(None, "dp", "group"),
        P("group", None),
        P("dp", None, None),
        P("dp", None),
        P("dp", None),
        P("dp", None),
    )
    out_specs = (P(None, "dp", "group"), P(("group", "dp"), None), P("dp", None))
    body = functools.partial(per_device, mesh.shape["group"], mesh.shape["dp"])
    if (mesh.shape["group"], mesh.shape["dp"]) == (4, 8):
        body = functools.partial(per_device_line, 4, 8)
    return jax.shard_map(
        body, mesh=mesh, in_specs=in_specs, out_specs=out_specs, check_vma=False
    )
```

```python
import functools

import jax
import jax.numpy as jnp
from jax import lax
from jax.experimental import pallas as pl
from jax.experimental.pallas import tpu as pltpu
from jax.sharding import PartitionSpec as P

discount_rate = 0.99
value_weight = 0.5
entropy_weight = 0.1
loss_divisor = 16.0


def contract_rows(left, right):
    return lax.dot_general(
        left, right, (((0,), (0,)), ((), ())), preferred_element_type=jnp.float32
    )


def contract_cols(left, right):
    return lax.dot_general(
        left, right, (((1,), (1,)), ((), ())), preferred_element_type=jnp.float32
    )


def silu_slope(pre_value):
    sigma = jax.nn.sigmoid(pre_value)
    return sigma * (1.0 + pre_value * (1.0 - sigma))


def importance_trace_gradients(
    learner_output, acting_policy_logits, actions, rewards, episode_finished
):
    log_behave = jax.nn.log_softmax(acting_policy_logits, axis=-1)
    chosen = actions[:, :, None] == jnp.arange(log_behave.shape[-1], dtype=jnp.int32)
    behave = jnp.sum(jnp.where(chosen, log_behave, 0.0), axis=-1)
    return trace_gradients(
        learner_output, behave, actions, rewards, episode_finished.astype(jnp.float32)
    )


def trace_gradients_packed(learner_output, packed):
    behave, actions, rewards, finished = packed
    return trace_gradients(learner_output, behave, actions.astype(jnp.int32), rewards, finished)


def trace_gradients(learner_output, behave, actions, rewards, finished):
    number_of_actions = learner_output.shape[-1] - 1
    logits = learner_output[:, :, :number_of_actions]
    values = learner_output[:, :, number_of_actions]
    log_policy = jax.nn.log_softmax(logits[:, :-1], axis=-1)
    chosen = (
        actions[:, :, None] == jnp.arange(number_of_actions, dtype=jnp.int32)[None, None, :]
    ).astype(jnp.float32)
    ratio = jnp.exp(jnp.sum(log_policy * chosen, axis=-1) - behave)
    clipped = jnp.minimum(ratio, 1.0)
    discount = discount_rate * (1.0 - finished)
    current = values[:, :-1]
    following = values[:, 1:]
    deltas = clipped * (rewards + discount * following - current)

    corrections, factors = deltas, discount * clipped
    reach, span = 1, deltas.shape[1]
    while reach < span:
        later = jnp.pad(corrections[:, reach:], ((0, 0), (0, reach)))
        later_factors = jnp.pad(factors[:, reach:], ((0, 0), (0, reach)))
        corrections = corrections + factors * later
        factors = factors * later_factors
        reach *= 2
    targets = current + corrections
    next_targets = jnp.concatenate([targets[:, 1:], values[:, -1:]], axis=1)
    advantage = clipped * (rewards + discount * next_targets - current)
    probability = jnp.exp(log_policy)
    entropy = -jnp.sum(probability * log_policy, axis=-1)
    logit_grad = (
        -advantage[..., None] * (chosen - probability)
        + entropy_weight * probability * (log_policy + entropy[..., None])
    ) / loss_divisor
    value_grad = -value_weight * (targets - current) / loss_divisor
    step_grad = jnp.concatenate([logit_grad, value_grad[..., None]], axis=-1)
    last_row = jnp.zeros((values.shape[0], 1, number_of_actions + 1), jnp.float32)
    return jnp.concatenate([step_grad, last_row], axis=1)


def swap(block, mask, size):
    return lax.ppermute(block, "group", [(index, index ^ mask) for index in range(size)])


def gather_features(block, size):
    if size != 4:
        return lax.all_gather(block, "group", axis=1, tiled=True)
    me = lax.axis_index("group")
    rows, width = block.shape
    half = rows // 2
    from_near = swap(block, 1, size)
    from_far = swap(block, 2, size)
    top = swap(from_near[:half], 2, size)
    bottom = swap(from_far[half:], 1, size)
    whole = jnp.zeros((rows, size * width), block.dtype)
    whole = lax.dynamic_update_slice(whole, block, (0, me * width))
    whole = lax.dynamic_update_slice(whole, from_near, (0, (me ^ 1) * width))
    whole = lax.dynamic_update_slice(whole, from_far, (0, (me ^ 2) * width))
    whole = lax.dynamic_update_slice(whole, top, (0, (me ^ 3) * width))
    return lax.dynamic_update_slice(whole, bottom, (half, (me ^ 3) * width))


def scatter_features(partial, size):
    if size != 4:
        return lax.psum_scatter(partial, "group", scatter_dimension=1, tiled=True)
    me = lax.axis_index("group")
    rows, width = partial.shape[0], partial.shape[1] // size
    half = rows // 2
    wire = jnp.bfloat16

    def part(start, mask):
        piece = lax.dynamic_slice(partial, (start, (me ^ mask) * width), (half, width))
        return piece

    def reduce_half(start, first, second):
        theirs = jnp.concatenate([part(start, first), part(start, 3)], axis=0)
        got = swap(theirs, first, size)
        onward = part(start, second).astype(jnp.float32) + got[half:].astype(jnp.float32)
        mine = part(start, 0).astype(jnp.float32) + got[:half].astype(jnp.float32)
        return mine + swap(onward.astype(wire), second, size).astype(jnp.float32)

    return jnp.concatenate([reduce_half(0, 1, 2), reduce_half(half, 2, 1)], axis=0)


def scatter_rows(block, size):
    if size & (size - 1):
        return lax.psum_scatter(block, "dp", scatter_dimension=0, tiled=True)
    me = lax.axis_index("dp")
    mask = size // 2
    while mask:
        half = block.shape[0] // 2
        upper = (me & mask) > 0
        theirs = jnp.where(upper, block[:half], block[half:])
        mine = jnp.where(upper, block[half:], block[:half])
        block = mine + lax.ppermute(theirs, "dp", [(i, i ^ mask) for i in range(size)])
        mask //= 2
    return block


def swap_cores(block, size):
    return lax.ppermute(block, "dp", [(index, index ^ 1) for index in range(size)])


def split_for_pair(whole, size):
    core = lax.axis_index("dp") % 2
    rows, width = whole.shape
    by_owner = whole.reshape(rows, size // 2, 2, width // size)

    def features_of(owner):
        picked = lax.dynamic_slice_in_dim(by_owner, owner, 1, axis=2)
        return picked.reshape(rows, width // 2)

    return features_of(core), swap_cores(features_of(1 - core), size)


def sum_group(block, size):
    if size != 4:
        return lax.psum(block, "group")
    block = block + swap(block, 1, size)
    return block + swap(block, 2, size)


def per_device(
    group_size,
    dp_size,
    observations,
    next_observations,
    trunk_weights,
    head_weights,
    acting_policy_logits,
    actions,
    rewards,
    episode_finished,
):
    traj_count, step_count, feature_block = observations.shape
    learner_rows = traj_count * step_count
    number_of_actions = acting_policy_logits.shape[-1]
    layer_total = trunk_weights.shape[0]
    own_rows = observations.reshape(learner_rows, feature_block)
    gathered_weights = [
        lax.all_gather(trunk_weights[layer_index], "dp", axis=0, tiled=True)
        for layer_index in range(layer_total)
    ]
    current = jnp.concatenate([own_rows, next_observations], axis=0)
    pair_inputs = []
    products_block = []
    for layer_index in range(layer_total):
        whole = gather_features(current, group_size)
        product = jnp.dot(
            whole, gathered_weights[layer_index], preferred_element_type=jnp.float32
        )
        pair_inputs.append(split_for_pair(whole[:learner_rows], dp_size))
        products_block.append(product[:learner_rows])
        current = jax.nn.silu(product).astype(jnp.bfloat16)
    partial_head = jnp.dot(current, head_weights, preferred_element_type=jnp.float32)
    totals = sum_group(partial_head, group_size)
    last_block = current[:learner_rows]
    head_out = totals[:learner_rows]
    actor_logits = totals[learner_rows:, :number_of_actions]
    learner_output = head_out.reshape(traj_count, step_count, number_of_actions + 1)
    output_gradient = importance_trace_gradients(
        learner_output, acting_policy_logits, actions, rewards, episode_finished
    )
    output_gradient = output_gradient.reshape(learner_rows, number_of_actions + 1).astype(
        jnp.bfloat16
    )
    input_grad = contract_cols(output_gradient, head_weights)
    grad_list = [None] * layer_total
    for layer_index in range(layer_total - 1, -1, -1):
        pre_grad = (input_grad * silu_slope(products_block[layer_index])).astype(jnp.bfloat16)
        near_inputs, far_inputs = pair_inputs[layer_index]
        far_grad = swap_cores(pre_grad, dp_size)
        partial = contract_rows(near_inputs, pre_grad) + contract_rows(far_inputs, far_grad)
        partial = partial.astype(jnp.bfloat16)
        partial, pre_grad = lax.optimization_barrier((partial, pre_grad))
        grad_list[layer_index] = lax.psum_scatter(
            partial,
            "dp",
            scatter_dimension=0,
            tiled=True,
            axis_index_groups=[list(range(core, dp_size, 2)) for core in range(2)],
        ).astype(jnp.float32)
        if layer_index > 0:
            full_grad = contract_cols(pre_grad, gathered_weights[layer_index]).astype(jnp.bfloat16)
            input_grad = scatter_features(full_grad, group_size)
    head_partial = contract_rows(last_block, output_gradient)
    head_grads = scatter_rows(head_partial, dp_size)
    return (jnp.stack(grad_list), head_grads, actor_logits)


MESH = pl.DeviceIdType.MESH
PIECES = 2
TILE = 256
PRODUCT_TILE = 512
VMEM_LIMIT = 67043328


class Place:
    def __init__(self):
        group, dp = lax.axis_index("group"), lax.axis_index("dp")
        self.group, self.dp = group, dp
        self.x, self.core, self.z = group % 2, dp % 2, dp // 2
        self.near_x = group + 1 - 2 * self.x
        self.near_y = (group + 2) % 4
        self.planes = lax.axis_size("dp") // 2
        self.to_x = (self.near_x, dp)
        self.to_y = (self.near_y, dp)
        self.to_core = (group, dp + 1 - 2 * self.core)
        self.to_way = ((group, dp + 2), (group, dp - 2))

    def source(self, way, far):
        return self.z - far if way == 0 else self.z + far

    def has_source(self, way, far):
        return self.z >= far if way == 0 else self.z + far < self.planes

    def has_next(self, way):
        return self.z + 1 < self.planes if way == 0 else self.z > 0

    def greet(self):
        barrier = pltpu.get_barrier_semaphore()
        for peer in (self.to_x, self.to_y, self.to_core):
            pl.semaphore_signal(barrier, inc=1, device_id=peer, device_id_type=MESH)
        for way in range(2):
            @pl.when(self.has_next(way))
            def _():
                pl.semaphore_signal(
                    barrier, inc=1, device_id=self.to_way[way], device_id_type=MESH)
        inner = jnp.logical_and(self.has_next(0), self.has_next(1))
        pl.semaphore_wait(barrier, jnp.where(inner, 5, 4))


def remote(source, target, sent, landed, peer):
    return pltpu.make_async_remote_copy(
        src_ref=source, dst_ref=target, send_sem=sent, recv_sem=landed,
        device_id=peer, device_id_type=MESH)


def step_kernel(
    outputs_used, observations, next_observations, weights, head_weights, packed,
    grads_out, head_grads_out, actor_out,
    weight_buf, input_buf, last_buf, total, pair_in, pair_grad, line, keep, first_out, first_in,
    second_out, second_in, head_send, head_land, head_pair, head_sum,
    local_sem, x_sent, x_landed, z_sent, z_landed, c_sent, c_landed, p_sent, p_landed,
    lz_sent, lz_landed, f_sent, f_landed, h_sent, h_landed, hl_sent, hl_landed, out_sem,
):
    place = Place()
    group, dp, z, core = place.group, place.dp, place.z, place.core
    layers, in_block, width = weights.shape
    learner_rows = observations.shape[0]
    rows = learner_rows + next_observations.shape[0]
    half = rows // 2
    piece_rows = in_block // PIECES
    halves = (pl.ds(0, half), pl.ds(half, half))

    loads = [
        pltpu.make_async_copy(
            observations, input_buf.at[0, group, pl.ds(0, learner_rows)], local_sem.at[0]),
        pltpu.make_async_copy(
            next_observations,
            input_buf.at[0, group, pl.ds(learner_rows, rows - learner_rows)], local_sem.at[1]),
    ] + [
        pltpu.make_async_copy(weights.at[layer], weight_buf.at[layer, dp], local_sem.at[2 + layer])
        for layer in range(layers)
    ]

    def weight_copy(layer, way, far, piece):
        block = 2 * place.source(way, far) + core
        span = weight_buf.at[layer, block, pl.ds(piece * piece_rows, piece_rows)]
        source = weights.at[layer, pl.ds(piece * piece_rows, piece_rows)] if far == 0 else span
        return remote(source, span, z_sent.at[layer, way, far, piece],
                      z_landed.at[layer, way, far, piece], place.to_way[way])

    def weight_arrival(layer, way, far, piece):
        block = 2 * place.source(way, far) + core
        span = weight_buf.at[layer, block, pl.ds(piece * piece_rows, piece_rows)]
        return remote(span, span, z_sent.at[layer, way, far - 1, piece],
                      z_landed.at[layer, way, far - 1, piece], place.to_core)

    def core_copy(layer, way, far, piece, arriving=False):
        owner = 1 - core if arriving else core
        block = 2 * place.source(way, far) + owner
        span = weight_buf.at[layer, block, pl.ds(piece * piece_rows, piece_rows)]
        source = span
        if far == 0 and not arriving:
            source = weights.at[layer, pl.ds(piece * piece_rows, piece_rows)]
        return remote(source, span, c_sent.at[layer, way, far, piece],
                      c_landed.at[layer, way, far, piece], place.to_core)

    def send_own_weights(layer, way):
        for piece in range(PIECES):
            weight_copy(layer, way, 0, piece).start()

    def send_own_core(layer):
        for piece in range(PIECES):
            core_copy(layer, 0, 0, piece).start()

    def own_turn(far):
        for way in range(2):
            edge = z == far if way == 0 else place.planes - 1 - z == far
            @pl.when(jnp.logical_and(edge, place.has_next(way)))
            def _():
                for layer in range(1, layers):
                    send_own_weights(layer, way)

    def relay(layer, far, piece):
        for way in range(2):
            @pl.when(place.has_source(way, far))
            def _():
                weight_arrival(layer, way, far, piece).wait_recv()
                @pl.when(place.has_next(way))
                def _():
                    weight_copy(layer, way, far, piece).start()
                core_copy(layer, way, far, piece).start()

    def input_copy(layer, stage, kind, arriving=False):
        lane, part = kind
        peer = (place.to_x, place.to_y)[lane]
        if stage == 0:
            quarter = (place.near_x, place.near_y)[lane] if arriving else group
        else:
            other = (place.near_y, place.near_x)[lane]
            quarter = (place.near_x + 2) % 4 if arriving else other
        span = input_buf.at[layer, quarter, halves[part]]
        index = (layer, stage, lane, part)
        return remote(span, span, x_sent.at[index], x_landed.at[index], peer)

    FIRST = ((0, 0), (1, 1))
    SECOND = ((0, 1), (1, 0))
    ONWARD = ((1, 0), (0, 1))

    def multiply(layer, plane):
        left = input_buf.at[layer, plane]
        right = weight_buf.at[layer, pl.ds(2 * plane, 2)]

        def step(tile, carry):
            columns = pl.ds(pl.multiple_of(tile * TILE, TILE), TILE)
            total[layer, :, columns] += jnp.dot(
                left[...], right[:, :, columns].reshape(width, TILE),
                preferred_element_type=jnp.float32)
            return carry
        lax.fori_loop(0, width // TILE, step, 0)

    def core_arrivals(layer, far):
        for way in range(2 if far else 1):
            def wait():
                for piece in range(PIECES):
                    core_copy(layer, way, far, piece, arriving=True).wait_recv()
            if far:
                pl.when(place.has_source(way, far))(wait)
            else:
                wait()

    def multiply_far(layer, far):
        core_arrivals(layer, far)
        if far == 0:
            multiply(layer, z)
            return
        for way in range(2):
            @pl.when(place.has_source(way, far))
            def _():
                multiply(layer, place.source(way, far))

    def finish(layer, part):
        span = halves[part]
        value = total[layer, span, :]
        result = (value * jax.nn.sigmoid(value)).astype(jnp.bfloat16)
        if layer + 1 < layers:
            input_buf[layer + 1, group, span, :] = result
        else:
            last_buf[span, :] = result

    other_cols = pl.ds(pl.multiple_of((1 - core) * in_block, in_block), in_block)

    def pair_inputs(layer):
        source = input_buf.at[layer, :, pl.ds(0, learner_rows), other_cols]
        return remote(source, pair_in.at[layer], p_sent.at[0, layer], p_landed.at[0, layer],
                      place.to_core)

    for load in loads:
        load.start()
    place.greet()
    for way in range(2):
        pl.when(place.has_next(way))(functools.partial(send_own_weights, 0, way))
    own_turn(0)
    loads[0].wait()
    loads[1].wait()
    for kind in FIRST + SECOND:
        input_copy(0, 0, kind).start()
    send_own_core(0)
    total[...] = jnp.zeros_like(total)
    for layer in range(layers):
        relay(layer, 1, 0)
        for kind in FIRST:
            input_copy(layer, 0, kind, True).wait_recv()
        for kind in ONWARD:
            input_copy(layer, 1, kind).start()
        for piece in range(1, PIECES):
            relay(layer, 1, piece)
        if layer == 0:
            own_turn(1)
        for kind in SECOND:
            input_copy(layer, 0, kind, True).wait_recv()
        relay(layer, 2, 0)
        for kind in ONWARD:
            input_copy(layer, 1, kind, True).wait_recv()
        pair_inputs(layer).start()
        if layer == 0:
            for load in loads[2:]:
                load.wait()
        multiply_far(layer, 0)
        for piece in range(1, PIECES):
            relay(layer, 2, piece)
        if layer == 0:
            own_turn(2)
            send_own_core(1)
        multiply_far(layer, 1)
        for piece in range(PIECES):
            relay(layer, 3, piece)
        multiply_far(layer, 2)
        multiply_far(layer, 3)
        for part in (0, 1):
            finish(layer, part)
            if layer + 1 < layers:
                for kind in FIRST + SECOND:
                    if kind[1] == part:
                        input_copy(layer + 1, 0, kind).start()

    planes = place.planes
    bhalf = learner_rows // 2
    bf16, f32 = jnp.bfloat16, jnp.float32
    top = layers - 1
    own_rows = pl.ds(pl.multiple_of(core * learner_rows, learner_rows), learner_rows)
    other_rows = pl.ds(pl.multiple_of((1 - core) * learner_rows, learner_rows), learner_rows)
    slot_width = width // (2 * planes)

    def pair_grads(layer, arriving=False):
        span = pair_grad.at[layer, other_rows if arriving else own_rows]
        return remote(span, span, p_sent.at[1, layer], p_landed.at[1, layer], place.to_core)

    def head_swap(arriving=False):
        return remote(head_pair.at[0], head_pair.at[1], h_sent.at[2], h_landed.at[2],
                      place.to_core)


    def small(stage, peer):
        return remote(head_send.at[stage], head_land.at[stage], h_sent.at[stage],
                      h_landed.at[stage], peer)

    outputs = head_weights.shape[0]
    partial_head = lax.dot_general(
        head_weights[...], last_buf[...], (((1,), (1,)), ((), ())), preferred_element_type=f32)
    for stage, peer in enumerate((place.to_x, place.to_y)):
        head_send[stage] = partial_head
        small(stage, peer).start()
        small(stage, peer).wait_recv()
        partial_head = head_send[stage] + head_land[stage]
    head_send[2] = partial_head
    actor_copy = pltpu.make_async_copy(
        head_send.at[2, :, pl.ds(learner_rows, rows - learner_rows)], actor_out, out_sem.at[0, PIECES])
    actor_copy.start()
    learner_head = head_send[2, :, :learner_rows]
    gradient = trace_columns(learner_head, packed[...], outputs_used - 1).astype(bf16)
    rows_each = learner_rows // 4
    for part in range(4):
        span = pl.ds(part * rows_each, rows_each)
        column = lax.dot_general(
            gradient[:, part * rows_each:(part + 1) * rows_each], head_weights[...],
            (((0,), (0,)), ((), ())), preferred_element_type=f32)
        value = total[top, span, :]
        sigma = jax.nn.sigmoid(value)
        slope = sigma * (1.0 + value * (1.0 - sigma))
        pair_grad[top, pl.ds(pl.multiple_of(core * learner_rows + part * rows_each, rows_each), rows_each), :] = (
            column * slope).astype(bf16)
    pair_grads(top).start()
    head_pair[0] = lax.dot_general(
        gradient, last_buf[pl.ds(0, learner_rows), :], (((1,), (0,)), ((), ())),
        preferred_element_type=f32)
    head_swap().start()

    lanes = ((place.to_x, place.to_y), (place.to_y, place.to_x))
    near = ((place.near_x, place.near_y), (place.near_y, place.near_x))
    far_quarter = (place.near_x + 2) % 4

    def first_copy(part, slot):
        index = (part, slot)
        return remote(first_out.at[index], first_in.at[index], f_sent.at[0, part, slot],
                      f_landed.at[0, part, slot], lanes[part][0])

    def second_copy(part):
        return remote(second_out.at[part], second_in.at[part], f_sent.at[1, part, 0],
                      f_landed.at[1, part, 0], lanes[part][1])

    def input_quarter(quarter, rows_of):
        parts = []
        for block in range(2):
            parts.append(lax.dot_general(
                pair_grad[top, rows_of, :], weight_buf[top, 2 * quarter + block],
                (((1,), (1,)), ((), ())), preferred_element_type=f32))
        return parts

    cores = pl.multiple_of(core * learner_rows, learner_rows)

    def rows_at(part):
        return pl.ds(pl.multiple_of(cores + part * bhalf, bhalf), bhalf)

    def block_cols(block):
        return pl.ds(block * in_block, in_block)

    def send_first(part, slot, quarter):
        for block, value in enumerate(input_quarter(quarter, rows_at(part))):
            first_out[part, slot, :, block_cols(block)] = value.astype(bf16)
        first_copy(part, slot).start()

    def keep_quarter(part, slot, quarter):
        for block, value in enumerate(input_quarter(quarter, rows_at(part))):
            keep[part, slot, :, block_cols(block)] = value

    def order(step):
        table = []
        for at in range(planes):
            up = list(range(planes - 1, at, -1))
            down = list(range(0, at))
            mixed = []
            while up or down:
                if up:
                    mixed.append(up.pop(0))
                if down:
                    mixed.append(down.pop(0))
            table.append((mixed + [at])[step])
        plane = table[-1]
        for at in range(planes - 1):
            plane = jnp.where(z == at, table[at], plane)
        return plane

    def line_send(layer, plane, piece, way):
        source = line.at[layer, plane, pl.ds(piece * piece_rows, piece_rows)]
        if way == 0:
            slot = plane
        else:
            slot = jnp.where(plane == z - 1, planes, plane)
        target = line.at[layer, slot, pl.ds(piece * piece_rows, piece_rows)]
        return remote(source, target, lz_sent.at[layer, plane, piece],
                      lz_landed.at[layer, slot, piece], place.to_way[way])

    def line_arrival(layer, slot, piece):
        span = line.at[layer, slot, pl.ds(piece * piece_rows, piece_rows)]
        return remote(span, span, lz_sent.at[layer, 0, piece],
                      lz_landed.at[layer, slot, piece], place.to_core)

    def product(layer, plane, piece, columns):
        contract = (((0,), (0,)), ((), ()))
        mine = pl.ds(pl.multiple_of(core * in_block + piece * piece_rows, piece_rows), piece_rows)
        value = lax.dot_general(
            input_buf[layer, plane, pl.ds(0, learner_rows), mine],
            pair_grad[layer, own_rows, columns], contract, preferred_element_type=f32)
        return value + lax.dot_general(
            pair_in[layer, plane, :, pl.ds(piece * piece_rows, piece_rows)],
            pair_grad[layer, other_rows, columns], contract, preferred_element_type=f32)

    tile = PRODUCT_TILE
    tiles = width // tile

    def over_tiles(body):
        def step(index, carry):
            body(pl.ds(pl.multiple_of(index * tile, tile), tile))
            return carry
        lax.fori_loop(0, tiles, step, 0)

    def pass_on(layer, step):
        plane = order(step)
        upward = plane > z
        fed = jnp.where(upward, z > 0, z + 1 < planes)
        for piece in range(PIECES):
            span = pl.ds(piece * piece_rows, piece_rows)

            @pl.when(fed)
            def _():
                line_arrival(layer, plane, piece).wait_recv()

                def body(columns):
                    value = product(layer, plane, piece, columns)
                    value = value + line[layer, plane, span, columns].astype(f32)
                    line[layer, plane, span, columns] = value.astype(bf16)
                over_tiles(body)

            @pl.when(jnp.logical_not(fed))
            def _():
                def body(columns):
                    value = product(layer, plane, piece, columns)
                    line[layer, plane, span, columns] = value.astype(bf16)
                over_tiles(body)

            pl.when(upward)(line_send(layer, plane, piece, 0).start)
            pl.when(jnp.logical_not(upward))(line_send(layer, plane, piece, 1).start)

    def head_line(plane, way, receiving):
        slot = plane
        if way == 1 and not receiving:
            slot = jnp.where(plane == z - 1, planes, plane)
        return remote(head_sum.at[plane], head_sum.at[slot], hl_sent.at[plane],
                      hl_landed.at[slot], place.to_core if receiving else place.to_way[way])

    def head_columns(which, plane):
        start = pl.multiple_of((2 * plane + core) * slot_width, slot_width)
        return head_pair[which, :, pl.ds(start, slot_width)]

    def head_pass(step):
        plane = order(step)
        upward = plane > z
        fed = jnp.where(upward, z > 0, z + 1 < planes)
        own = head_columns(0, plane) + head_columns(1, plane)

        @pl.when(fed)
        def _():
            head_line(plane, 0, True).wait_recv()
            head_sum[plane] = head_sum[plane] + own

        @pl.when(jnp.logical_not(fed))
        def _():
            head_sum[plane] = own

        pl.when(upward)(head_line(plane, 0, False).start)
        pl.when(jnp.logical_not(upward))(head_line(plane, 1, False).start)

    def head_final():
        head_land[0, :, pl.ds(0, slot_width)] = head_columns(0, z) + head_columns(1, z)
        for slot, present in ((z, z > 0), (planes, z + 1 < planes)):
            @pl.when(present)
            def _():
                head_line(slot, 0, True).wait_recv()
                head_land[0, :, pl.ds(0, slot_width)] += head_sum[slot]
        pltpu.make_async_copy(
            head_land.at[0, :, pl.ds(0, slot_width)], head_grads_out, out_sem.at[1, PIECES]).start()

    def drain(layer, step):
        plane = order(step)
        for piece in range(PIECES):
            span = line.at[layer, plane, pl.ds(piece * piece_rows, piece_rows)]
            remote(span, span, lz_sent.at[layer, plane, piece],
                   lz_landed.at[layer, plane, piece], place.to_core).wait_send()

    def own_product(layer):
        for piece in range(PIECES):
            span = pl.ds(piece * piece_rows, piece_rows)

            def body(columns):
                total[layer, span, columns] = product(layer, z, piece, columns)
            over_tiles(body)

    def own_add(layer):
        for piece in range(PIECES):
            span = pl.ds(piece * piece_rows, piece_rows)
            for slot, present in ((z, z > 0), (planes, z + 1 < planes)):
                @pl.when(present)
                def _():
                    line_arrival(layer, slot, piece).wait_recv()
                    total[layer, span, :] += line[layer, slot, span, :].astype(f32)
            pltpu.make_async_copy(
                total.at[layer, span], grads_out.at[layer, span],
                out_sem.at[layer, piece]).start()


    for part in range(2):
        send_first(part, 0, far_quarter)
    pair_grads(top, True).wait_recv()
    pair_inputs(top).wait_recv()
    outer = jnp.logical_or(z == 0, z == planes - 1)
    pl.when(outer)(functools.partial(pass_on, top, 0))
    for part in range(2):
        send_first(part, 1, near[part][0])
    for part in range(2):
        keep_quarter(part, 1, near[part][1])
        keep_quarter(part, 0, group)
    pl.when(jnp.logical_not(outer))(functools.partial(pass_on, top, 0))
    head_swap(True).wait_recv()
    head_pass(0)
    for part in range(2):
        first_copy(part, 0).wait_recv()
        second_out[part] = (keep[part, 1] + first_in[part, 0].astype(f32)).astype(bf16)
        second_copy(part).start()
    pass_on(top, 1)
    head_pass(1)
    for part in range(2):
        first_copy(part, 1).wait_recv()
        second_copy(part).wait_recv()
        summed = keep[part, 0] + first_in[part, 1].astype(f32) + second_in[part].astype(f32)
        value = total[0, pl.ds(part * bhalf, bhalf), :]
        sigma = jax.nn.sigmoid(value)
        slope = sigma * (1.0 + value * (1.0 - sigma))
        pair_grad[0, rows_at(part), :] = (summed * slope).astype(bf16)
    pair_grads(0).start()
    pass_on(top, 2)
    head_pass(2)
    own_product(top)
    pair_grads(0, True).wait_recv()
    pair_inputs(0).wait_recv()
    pass_on(0, 0)
    own_add(top)
    head_final()
    pass_on(0, 1)
    own_product(0)
    pass_on(0, 2)
    own_add(0)

    for layer in range(layers):
        pair_inputs(layer).wait_send()
        pair_grads(layer).wait_send()
        for step in range(planes - 1):
            drain(layer, step)
        for piece in range(PIECES):
            span = pl.ds(piece * piece_rows, piece_rows)
            pltpu.make_async_copy(
                total.at[layer, span], grads_out.at[layer, span],
                out_sem.at[layer, piece]).wait()
    for part in range(2):
        for slot in range(2):
            first_copy(part, slot).wait_send()
        second_copy(part).wait_send()
    small(0, place.to_x).wait_send()
    small(1, place.to_y).wait_send()
    head_swap().wait_send()
    for step in range(planes - 1):
        head_line(order(step), 0, True).wait_send()
    actor_copy.wait()
    pltpu.make_async_copy(
        head_land.at[0, :, pl.ds(0, slot_width)], head_grads_out, out_sem.at[1, PIECES]).wait()

    for layer in range(layers):
        for kind in FIRST + SECOND:
            input_copy(layer, 0, kind).wait_send()
        for kind in ONWARD:
            input_copy(layer, 1, kind).wait_send()
        for piece in range(PIECES):
            core_copy(layer, 0, 0, piece).wait_send()
            for way in range(2):
                pl.when(place.has_next(way))(weight_copy(layer, way, 0, piece).wait_send)
                for far in (1, 2, 3):
                    @pl.when(place.has_source(way, far))
                    def _():
                        pl.when(place.has_next(way))(
                            weight_copy(layer, way, far, piece).wait_send)
                        core_copy(layer, way, far, piece).wait_send()

def trace_columns(outputs, packed, actions_total):
    count, columns = outputs.shape
    row = lax.broadcasted_iota(jnp.int32, (count, columns), 0)
    is_action = row < actions_total
    behave, action = packed[0:1], packed[1:2]
    rewards, finished, live = packed[2:3], packed[3:4], packed[4:5]

    def after(value, reach):
        return pltpu.roll(value, columns - reach, 1)

    peak = jnp.max(jnp.where(is_action, outputs, -jnp.inf), axis=0, keepdims=True)
    shifted = jnp.where(is_action, outputs - peak, 0.0)
    weight = jnp.where(is_action, jnp.exp(shifted), 0.0)
    scale = jnp.sum(weight, axis=0, keepdims=True)
    log_policy = jnp.where(is_action, shifted - jnp.log(scale), 0.0)
    probability = jnp.where(is_action, jnp.exp(log_policy), 0.0)
    chosen = jnp.where(row == action.astype(jnp.int32), 1.0, 0.0)
    ratio = jnp.exp(jnp.sum(log_policy * chosen, axis=0, keepdims=True) - behave)
    clipped = jnp.minimum(ratio, 1.0)
    discount = discount_rate * (1.0 - finished)
    current = jnp.sum(jnp.where(row == actions_total, outputs, 0.0), axis=0, keepdims=True)
    corrections = live * clipped * (rewards + discount * after(current, 1) - current)
    factors = live * discount * clipped
    reach = 1
    while reach < columns:
        corrections = corrections + factors * after(corrections, reach)
        factors = factors * after(factors, reach)
        reach *= 2
    targets = current + corrections
    advantage = clipped * (rewards + discount * after(targets, 1) - current)
    entropy = -jnp.sum(probability * log_policy, axis=0, keepdims=True)
    logit_grad = (
        -advantage * (chosen - probability)
        + entropy_weight * probability * (log_policy + entropy)
    ) / loss_divisor
    value_grad = -value_weight * (targets - current) / loss_divisor
    result = jnp.where(is_action, logit_grad, jnp.where(row == actions_total, value_grad, 0.0))
    return jnp.where(live > 0.0, result, 0.0)


def whole_step(observations, next_observations, weights, head_weights, packed, outputs_used):
    layers, in_block, width = weights.shape
    learner_rows = observations.shape[0]
    rows = learner_rows + next_observations.shape[0]
    padded = head_weights.shape[0]
    planes = lax.axis_size("dp") // 2
    bf16, f32 = jnp.bfloat16, jnp.float32
    half = learner_rows // 2
    dma = pltpu.SemaphoreType.DMA
    hbm = pl.BlockSpec(memory_space=pltpu.HBM)
    vmem = pl.BlockSpec(memory_space=pltpu.VMEM)
    slot_width = width // (2 * planes)
    return pl.pallas_call(
        functools.partial(step_kernel, outputs_used),
        out_shape=(
            jax.ShapeDtypeStruct((layers, in_block, width), f32),
            jax.ShapeDtypeStruct((padded, slot_width), f32),
            jax.ShapeDtypeStruct((padded, rows - learner_rows), f32),
        ),
        in_specs=[hbm] * 3 + [vmem] * 2,
        out_specs=(hbm,) * 3,
        scratch_shapes=[
            pltpu.VMEM((layers, 2 * planes, in_block, width), bf16),
            pltpu.VMEM((layers, 4, rows, width), bf16),
            pltpu.VMEM((rows, width), bf16),
            pltpu.VMEM((layers, rows, width), f32),
            pltpu.VMEM((layers, 4, learner_rows, in_block), bf16),
            pltpu.VMEM((layers, 2 * learner_rows, width), bf16),
            pltpu.VMEM((layers, planes + 1, in_block, width), bf16),
            pltpu.VMEM((2, 2, half, width), f32),
            pltpu.VMEM((2, 2, half, width), bf16),
            pltpu.VMEM((2, 2, half, width), bf16),
            pltpu.VMEM((2, half, width), bf16),
            pltpu.VMEM((2, half, width), bf16),
            pltpu.VMEM((3, padded, rows), f32),
            pltpu.VMEM((2, padded, rows), f32),
            pltpu.VMEM((2, padded, width), f32),
            pltpu.VMEM((planes + 1, padded, slot_width), f32),
            dma((2 + layers,)),
            dma((layers, 2, 2, 2)), dma((layers, 2, 2, 2)),
            dma((layers, 2, 4, PIECES)), dma((layers, 2, 4, PIECES)),
            dma((layers, 2, 4, PIECES)), dma((layers, 2, 4, PIECES)),
            dma((2, layers)), dma((2, layers)),
            dma((layers, planes + 1, PIECES)), dma((layers, planes + 1, PIECES)),
            dma((2, 2, 2)), dma((2, 2, 2)),
            dma((3,)), dma((3,)),
            dma((planes + 1,)), dma((planes + 1,)),
            dma((layers, PIECES + 1)),
        ],
        compiler_params=pltpu.CompilerParams(
            collective_id=0, has_side_effects=True, vmem_limit_bytes=VMEM_LIMIT),
        name="learner_step",
    )(observations, next_observations, weights, head_weights, packed)


def per_device_line(
    observations, next_observations, trunk_weights, head_weights,
    acting_policy_logits, actions, rewards, episode_finished,
):
    traj_count, step_count, feature_block = observations.shape
    learner_rows = traj_count * step_count
    number_of_actions = acting_policy_logits.shape[-1]
    used = number_of_actions + 1
    f32 = jnp.float32
    log_behave = jax.nn.log_softmax(acting_policy_logits, axis=-1)
    chosen = actions[:, :, None] == jnp.arange(number_of_actions, dtype=jnp.int32)
    behave = jnp.sum(jnp.where(chosen, log_behave, 0.0), axis=-1)
    packed = jnp.stack([
        behave, actions.astype(f32), rewards, episode_finished.astype(f32),
        jnp.ones_like(behave)])
    packed = jnp.pad(packed, ((0, 3), (0, 0), (0, 1))).reshape(8, learner_rows)
    padded = -(-used // 16) * 16
    head_rows = jnp.pad(head_weights.T, ((0, padded - used), (0, 0)))
    trunk_grads, head_grads, actor_logits = whole_step(
        observations.reshape(learner_rows, feature_block), next_observations, trunk_weights,
        head_rows, packed, used)
    return trunk_grads, head_grads[:used].T, actor_logits[:number_of_actions].T


def solution(mesh):
    in_specs = (
        P("dp", None, "group"),
        P("dp", "group"),
        P(None, "dp", "group"),
        P("group", None),
        P("dp", None, None),
        P("dp", None),
        P("dp", None),
        P("dp", None),
    )
    out_specs = (P(None, "dp", "group"), P(("group", "dp"), None), P("dp", None))
    body = functools.partial(per_device, mesh.shape["group"], mesh.shape["dp"])
    if (mesh.shape["group"], mesh.shape["dp"]) == (4, 8):
        body = per_device_line
    return jax.shard_map(
        body, mesh=mesh, in_specs=in_specs, out_specs=out_specs, check_vma=False
    )
```

```python
import functools

import jax
import jax.numpy as jnp
from jax import lax
from jax.experimental import pallas as pl
from jax.experimental.pallas import tpu as pltpu
from jax.sharding import PartitionSpec as P

discount_rate = 0.99
value_weight = 0.5
entropy_weight = 0.1
loss_divisor = 16.0


def contract_rows(left, right):
    return lax.dot_general(
        left, right, (((0,), (0,)), ((), ())), preferred_element_type=jnp.float32
    )


def contract_cols(left, right):
    return lax.dot_general(
        left, right, (((1,), (1,)), ((), ())), preferred_element_type=jnp.float32
    )


def silu_slope(pre_value):
    sigma = jax.nn.sigmoid(pre_value)
    return sigma * (1.0 + pre_value * (1.0 - sigma))


def importance_trace_gradients(
    learner_output, acting_policy_logits, actions, rewards, episode_finished
):
    log_behave = jax.nn.log_softmax(acting_policy_logits, axis=-1)
    chosen = actions[:, :, None] == jnp.arange(log_behave.shape[-1], dtype=jnp.int32)
    behave = jnp.sum(jnp.where(chosen, log_behave, 0.0), axis=-1)
    return trace_gradients(
        learner_output, behave, actions, rewards, episode_finished.astype(jnp.float32)
    )


def trace_gradients_packed(learner_output, packed):
    behave, actions, rewards, finished = packed
    return trace_gradients(learner_output, behave, actions.astype(jnp.int32), rewards, finished)


def trace_gradients(learner_output, behave, actions, rewards, finished):
    number_of_actions = learner_output.shape[-1] - 1
    logits = learner_output[:, :, :number_of_actions]
    values = learner_output[:, :, number_of_actions]
    log_policy = jax.nn.log_softmax(logits[:, :-1], axis=-1)
    chosen = (
        actions[:, :, None] == jnp.arange(number_of_actions, dtype=jnp.int32)[None, None, :]
    ).astype(jnp.float32)
    ratio = jnp.exp(jnp.sum(log_policy * chosen, axis=-1) - behave)
    clipped = jnp.minimum(ratio, 1.0)
    discount = discount_rate * (1.0 - finished)
    current = values[:, :-1]
    following = values[:, 1:]
    deltas = clipped * (rewards + discount * following - current)

    corrections, factors = deltas, discount * clipped
    reach, span = 1, deltas.shape[1]
    while reach < span:
        later = jnp.pad(corrections[:, reach:], ((0, 0), (0, reach)))
        later_factors = jnp.pad(factors[:, reach:], ((0, 0), (0, reach)))
        corrections = corrections + factors * later
        factors = factors * later_factors
        reach *= 2
    targets = current + corrections
    next_targets = jnp.concatenate([targets[:, 1:], values[:, -1:]], axis=1)
    advantage = clipped * (rewards + discount * next_targets - current)
    probability = jnp.exp(log_policy)
    entropy = -jnp.sum(probability * log_policy, axis=-1)
    logit_grad = (
        -advantage[..., None] * (chosen - probability)
        + entropy_weight * probability * (log_policy + entropy[..., None])
    ) / loss_divisor
    value_grad = -value_weight * (targets - current) / loss_divisor
    step_grad = jnp.concatenate([logit_grad, value_grad[..., None]], axis=-1)
    last_row = jnp.zeros((values.shape[0], 1, number_of_actions + 1), jnp.float32)
    return jnp.concatenate([step_grad, last_row], axis=1)


def swap(block, mask, size):
    return lax.ppermute(block, "group", [(index, index ^ mask) for index in range(size)])


def gather_features(block, size):
    if size != 4:
        return lax.all_gather(block, "group", axis=1, tiled=True)
    me = lax.axis_index("group")
    rows, width = block.shape
    half = rows // 2
    from_near = swap(block, 1, size)
    from_far = swap(block, 2, size)
    top = swap(from_near[:half], 2, size)
    bottom = swap(from_far[half:], 1, size)
    whole = jnp.zeros((rows, size * width), block.dtype)
    whole = lax.dynamic_update_slice(whole, block, (0, me * width))
    whole = lax.dynamic_update_slice(whole, from_near, (0, (me ^ 1) * width))
    whole = lax.dynamic_update_slice(whole, from_far, (0, (me ^ 2) * width))
    whole = lax.dynamic_update_slice(whole, top, (0, (me ^ 3) * width))
    return lax.dynamic_update_slice(whole, bottom, (half, (me ^ 3) * width))


def scatter_features(partial, size):
    if size != 4:
        return lax.psum_scatter(partial, "group", scatter_dimension=1, tiled=True)
    me = lax.axis_index("group")
    rows, width = partial.shape[0], partial.shape[1] // size
    half = rows // 2
    wire = jnp.bfloat16

    def part(start, mask):
        piece = lax.dynamic_slice(partial, (start, (me ^ mask) * width), (half, width))
        return piece

    def reduce_half(start, first, second):
        theirs = jnp.concatenate([part(start, first), part(start, 3)], axis=0)
        got = swap(theirs, first, size)
        onward = part(start, second).astype(jnp.float32) + got[half:].astype(jnp.float32)
        mine = part(start, 0).astype(jnp.float32) + got[:half].astype(jnp.float32)
        return mine + swap(onward.astype(wire), second, size).astype(jnp.float32)

    return jnp.concatenate([reduce_half(0, 1, 2), reduce_half(half, 2, 1)], axis=0)


def scatter_rows(block, size):
    if size & (size - 1):
        return lax.psum_scatter(block, "dp", scatter_dimension=0, tiled=True)
    me = lax.axis_index("dp")
    mask = size // 2
    while mask:
        half = block.shape[0] // 2
        upper = (me & mask) > 0
        theirs = jnp.where(upper, block[:half], block[half:])
        mine = jnp.where(upper, block[half:], block[:half])
        block = mine + lax.ppermute(theirs, "dp", [(i, i ^ mask) for i in range(size)])
        mask //= 2
    return block


def swap_cores(block, size):
    return lax.ppermute(block, "dp", [(index, index ^ 1) for index in range(size)])


def split_for_pair(whole, size):
    core = lax.axis_index("dp") % 2
    rows, width = whole.shape
    by_owner = whole.reshape(rows, size // 2, 2, width // size)

    def features_of(owner):
        picked = lax.dynamic_slice_in_dim(by_owner, owner, 1, axis=2)
        return picked.reshape(rows, width // 2)

    return features_of(core), swap_cores(features_of(1 - core), size)


def sum_group(block, size):
    if size != 4:
        return lax.psum(block, "group")
    block = block + swap(block, 1, size)
    return block + swap(block, 2, size)


def per_device(
    group_size,
    dp_size,
    observations,
    next_observations,
    trunk_weights,
    head_weights,
    acting_policy_logits,
    actions,
    rewards,
    episode_finished,
):
    traj_count, step_count, feature_block = observations.shape
    learner_rows = traj_count * step_count
    number_of_actions = acting_policy_logits.shape[-1]
    layer_total = trunk_weights.shape[0]
    own_rows = observations.reshape(learner_rows, feature_block)
    gathered_weights = [
        lax.all_gather(trunk_weights[layer_index], "dp", axis=0, tiled=True)
        for layer_index in range(layer_total)
    ]
    current = jnp.concatenate([own_rows, next_observations], axis=0)
    pair_inputs = []
    products_block = []
    for layer_index in range(layer_total):
        whole = gather_features(current, group_size)
        product = jnp.dot(
            whole, gathered_weights[layer_index], preferred_element_type=jnp.float32
        )
        pair_inputs.append(split_for_pair(whole[:learner_rows], dp_size))
        products_block.append(product[:learner_rows])
        current = jax.nn.silu(product).astype(jnp.bfloat16)
    partial_head = jnp.dot(current, head_weights, preferred_element_type=jnp.float32)
    totals = sum_group(partial_head, group_size)
    last_block = current[:learner_rows]
    head_out = totals[:learner_rows]
    actor_logits = totals[learner_rows:, :number_of_actions]
    learner_output = head_out.reshape(traj_count, step_count, number_of_actions + 1)
    output_gradient = importance_trace_gradients(
        learner_output, acting_policy_logits, actions, rewards, episode_finished
    )
    output_gradient = output_gradient.reshape(learner_rows, number_of_actions + 1).astype(
        jnp.bfloat16
    )
    input_grad = contract_cols(output_gradient, head_weights)
    grad_list = [None] * layer_total
    for layer_index in range(layer_total - 1, -1, -1):
        pre_grad = (input_grad * silu_slope(products_block[layer_index])).astype(jnp.bfloat16)
        near_inputs, far_inputs = pair_inputs[layer_index]
        far_grad = swap_cores(pre_grad, dp_size)
        partial = contract_rows(near_inputs, pre_grad) + contract_rows(far_inputs, far_grad)
        partial = partial.astype(jnp.bfloat16)
        partial, pre_grad = lax.optimization_barrier((partial, pre_grad))
        grad_list[layer_index] = lax.psum_scatter(
            partial,
            "dp",
            scatter_dimension=0,
            tiled=True,
            axis_index_groups=[list(range(core, dp_size, 2)) for core in range(2)],
        ).astype(jnp.float32)
        if layer_index > 0:
            full_grad = contract_cols(pre_grad, gathered_weights[layer_index]).astype(jnp.bfloat16)
            input_grad = scatter_features(full_grad, group_size)
    head_partial = contract_rows(last_block, output_gradient)
    head_grads = scatter_rows(head_partial, dp_size)
    return (jnp.stack(grad_list), head_grads, actor_logits)


MESH = pl.DeviceIdType.MESH
PIECES = 2
TILE = 256
PRODUCT_TILE = 512
VMEM_LIMIT = 67043328


class Place:
    def __init__(self):
        group, dp = lax.axis_index("group"), lax.axis_index("dp")
        self.group, self.dp = group, dp
        self.x, self.core, self.z = group % 2, dp % 2, dp // 2
        self.near_x = group + 1 - 2 * self.x
        self.near_y = (group + 2) % 4
        self.planes = lax.axis_size("dp") // 2
        self.to_x = (self.near_x, dp)
        self.to_y = (self.near_y, dp)
        self.to_core = (group, dp + 1 - 2 * self.core)
        self.to_way = ((group, dp + 2), (group, dp - 2))
        self.mate = self.z + 1 - 2 * (self.z % 2)
        self.to_mate = (group, 2 * self.mate + self.core)
        self.outer = jnp.logical_or(self.z == 0, self.z == self.planes - 1)
        self.inner = jnp.logical_not(self.outer)

    def source(self, way, far):
        return self.z - far if way == 0 else self.z + far

    def has_source(self, way, far):
        return self.z >= far if way == 0 else self.z + far < self.planes

    def has_next(self, way):
        return self.z + 1 < self.planes if way == 0 else self.z > 0

    def greet(self):
        barrier = pltpu.get_barrier_semaphore()
        for peer in (self.to_x, self.to_y, self.to_core):
            pl.semaphore_signal(barrier, inc=1, device_id=peer, device_id_type=MESH)
        for way in range(2):
            @pl.when(self.has_next(way))
            def _():
                pl.semaphore_signal(
                    barrier, inc=1, device_id=self.to_way[way], device_id_type=MESH)
        inner = jnp.logical_and(self.has_next(0), self.has_next(1))
        pl.semaphore_wait(barrier, jnp.where(inner, 5, 4))


def remote(source, target, sent, landed, peer):
    return pltpu.make_async_remote_copy(
        src_ref=source, dst_ref=target, send_sem=sent, recv_sem=landed,
        device_id=peer, device_id_type=MESH)


def step_kernel(
    observations, next_observations, weights, head_raw, acting_raw, actions_raw, rewards_raw,
    finished_raw, grads_out, head_grads_out, actor_out,
    weight_buf, input_buf, last_buf, total, pair_in, pair_grad, line, keep, ship, stage, head_send, head_land, head_pair, head_sum, head_own, acting_own,
    actions_own, rewards_own, finished_own, head_weights, packed, head_result, actor_result,
    local_sem, x_sent, x_landed, z_sent, z_landed, c_sent, c_landed, p_sent, p_landed,
    lz_sent, lz_landed, f_sent, f_landed, h_sent, h_landed, hl_sent, hl_landed, s_sent, s_landed, out_sem,
):
    place = Place()
    group, dp, z, core = place.group, place.dp, place.z, place.core
    layers, in_block, width = weights.shape
    learner_rows = observations.shape[0]
    rows = learner_rows + next_observations.shape[0]
    half = rows // 2
    piece_rows = in_block // PIECES
    halves = (pl.ds(0, half), pl.ds(half, half))

    loads = [
        pltpu.make_async_copy(
            observations, input_buf.at[0, group, pl.ds(0, learner_rows)], local_sem.at[0]),
        pltpu.make_async_copy(
            next_observations,
            input_buf.at[0, group, pl.ds(learner_rows, rows - learner_rows)], local_sem.at[1]),
    ] + [
        pltpu.make_async_copy(weights.at[layer], weight_buf.at[layer, dp], local_sem.at[2 + layer])
        for layer in range(layers)
    ]

    def weight_copy(layer, way, far, piece):
        block = 2 * place.source(way, far) + core
        span = weight_buf.at[layer, block, pl.ds(piece * piece_rows, piece_rows)]
        source = weights.at[layer, pl.ds(piece * piece_rows, piece_rows)] if far == 0 else span
        return remote(source, span, z_sent.at[layer, way, far, piece],
                      z_landed.at[layer, way, far, piece], place.to_way[way])

    def weight_arrival(layer, way, far, piece):
        block = 2 * place.source(way, far) + core
        span = weight_buf.at[layer, block, pl.ds(piece * piece_rows, piece_rows)]
        return remote(span, span, z_sent.at[layer, way, far - 1, piece],
                      z_landed.at[layer, way, far - 1, piece], place.to_core)

    def core_copy(layer, way, far, piece, arriving=False):
        owner = 1 - core if arriving else core
        block = 2 * place.source(way, far) + owner
        span = weight_buf.at[layer, block, pl.ds(piece * piece_rows, piece_rows)]
        source = span
        if far == 0 and not arriving:
            source = weights.at[layer, pl.ds(piece * piece_rows, piece_rows)]
        return remote(source, span, c_sent.at[layer, way, far, piece],
                      c_landed.at[layer, way, far, piece], place.to_core)

    def send_own_weights(layer, way):
        for piece in range(PIECES):
            weight_copy(layer, way, 0, piece).start()

    def send_own_core(layer):
        for piece in range(PIECES):
            core_copy(layer, 0, 0, piece).start()

    def own_turn(far):
        for way in range(2):
            edge = z == far if way == 0 else place.planes - 1 - z == far
            @pl.when(jnp.logical_and(edge, place.has_next(way)))
            def _():
                for layer in range(1, layers):
                    send_own_weights(layer, way)

    def relay(layer, far, piece):
        for way in range(2):
            @pl.when(place.has_source(way, far))
            def _():
                weight_arrival(layer, way, far, piece).wait_recv()
                @pl.when(place.has_next(way))
                def _():
                    weight_copy(layer, way, far, piece).start()
                core_copy(layer, way, far, piece).start()

    def input_copy(layer, stage, kind, arriving=False):
        lane, part = kind
        peer = (place.to_x, place.to_y)[lane]
        if stage == 0:
            quarter = (place.near_x, place.near_y)[lane] if arriving else group
        else:
            other = (place.near_y, place.near_x)[lane]
            quarter = (place.near_x + 2) % 4 if arriving else other
        span = input_buf.at[layer, quarter, halves[part]]
        index = (layer, stage, lane, part)
        return remote(span, span, x_sent.at[index], x_landed.at[index], peer)

    FIRST = ((0, 0), (1, 1))
    SECOND = ((0, 1), (1, 0))
    ONWARD = ((1, 0), (0, 1))

    def multiply(layer, plane):
        left = input_buf.at[layer, plane]
        right = weight_buf.at[layer, pl.ds(2 * plane, 2)]

        def step(tile, carry):
            columns = pl.ds(pl.multiple_of(tile * TILE, TILE), TILE)
            total[layer, :, columns] += jnp.dot(
                left[...], right[:, :, columns].reshape(width, TILE),
                preferred_element_type=jnp.float32)
            return carry
        lax.fori_loop(0, width // TILE, step, 0)

    def core_arrivals(layer, far):
        for way in range(2 if far else 1):
            def wait():
                for piece in range(PIECES):
                    core_copy(layer, way, far, piece, arriving=True).wait_recv()
            if far:
                pl.when(place.has_source(way, far))(wait)
            else:
                wait()

    def multiply_far(layer, far):
        core_arrivals(layer, far)
        if far == 0:
            multiply(layer, z)
            return
        for way in range(2):
            @pl.when(place.has_source(way, far))
            def _():
                multiply(layer, place.source(way, far))

    def finish(layer, part):
        span = halves[part]
        value = total[layer, span, :]
        result = (value * jax.nn.sigmoid(value)).astype(jnp.bfloat16)
        if layer + 1 < layers:
            input_buf[layer + 1, group, span, :] = result
        else:
            last_buf[span, :] = result

    other_cols = pl.ds(pl.multiple_of((1 - core) * in_block, in_block), in_block)

    def pair_inputs(layer):
        source = input_buf.at[layer, :, pl.ds(0, learner_rows), other_cols]
        return remote(source, pair_in.at[layer], p_sent.at[0, layer], p_landed.at[0, layer],
                      place.to_core)

    side = [
        pltpu.make_async_copy(source, target, local_sem.at[2 + layers + index])
        for index, (source, target) in enumerate((
            (head_raw, head_own), (acting_raw, acting_own), (actions_raw, actions_own),
            (rewards_raw, rewards_own), (finished_raw, finished_own)))
    ]
    own_cols = pl.ds(pl.multiple_of(core * in_block, in_block), in_block)
    owner_rows = (pl.ds(0, learner_rows), pl.ds(learner_rows, learner_rows))
    core_rows = pl.ds(pl.multiple_of(core * learner_rows, learner_rows), learner_rows)
    mate_rows = pl.ds(pl.multiple_of((1 - core) * learner_rows, learner_rows), learner_rows)

    whole_stage = stage.at[pl.ds(0, learner_rows)]

    def ship_copy(other):
        source = input_buf.at[1, group, pl.ds(0, learner_rows), other_cols if other else own_cols]
        target = whole_stage if other else ship.at[group, core_rows]
        return remote(source, target, s_sent.at[other], s_landed.at[other], place.to_mate)

    def stage_copy(arriving=False):
        return remote(whole_stage, ship.at[group, mate_rows if arriving else core_rows],
                      s_sent.at[2], s_landed.at[2], place.to_core)

    def spread_copy(level, kind, arriving=False):
        lane, part = kind
        peer = (place.to_x, place.to_y)[lane]
        if level == 0:
            quarter = (place.near_x, place.near_y)[lane] if arriving else group
        else:
            other = (place.near_y, place.near_x)[lane]
            quarter = (place.near_x + 2) % 4 if arriving else other
        span = ship.at[quarter, owner_rows[part]]
        index = 3 + level * 4 + lane * 2 + part
        return remote(span, span, s_sent.at[index], s_landed.at[index], peer)

    def grad_ship(piece):
        step = learner_rows // 2
        source = pair_grad.at[layers - 1, pl.ds(
            pl.multiple_of(core * learner_rows + piece * step, step), step)]
        target = weight_buf.at[0, 6 + core, pl.ds(piece * step, step)]
        return remote(source, target, s_sent.at[11 + piece], s_landed.at[11 + piece],
                      place.to_mate)

    def grad_swap(piece, arriving=False):
        step = learner_rows // 2
        owner = 1 - core if arriving else core
        span = weight_buf.at[0, 6 + owner, pl.ds(piece * step, step)]
        return remote(span, span, s_sent.at[13 + piece], s_landed.at[13 + piece], place.to_core)

    def drain_weights(layer):
        for piece in range(PIECES):
            core_copy(layer, 0, 0, piece).wait_send()
            for way in range(2):
                pl.when(place.has_next(way))(weight_copy(layer, way, 0, piece).wait_send)
                for far in (1, 2, 3):
                    @pl.when(place.has_source(way, far))
                    def _():
                        pl.when(place.has_next(way))(
                            weight_copy(layer, way, far, piece).wait_send)
                        core_copy(layer, way, far, piece).wait_send()

    for load in loads + side:
        load.start()
    place.greet()
    for way in range(2):
        pl.when(place.has_next(way))(functools.partial(send_own_weights, 0, way))
    own_turn(0)
    loads[0].wait()
    loads[1].wait()
    for kind in FIRST + SECOND:
        input_copy(0, 0, kind).start()
    send_own_core(0)
    total[...] = jnp.zeros_like(total)
    for copy in side:
        copy.wait()
    prepare(head_own, acting_own, actions_own, rewards_own, finished_own, head_weights, packed)
    for layer in range(layers):
        relay(layer, 1, 0)
        for kind in FIRST:
            input_copy(layer, 0, kind, True).wait_recv()
        for kind in ONWARD:
            input_copy(layer, 1, kind).start()
        for piece in range(1, PIECES):
            relay(layer, 1, piece)
        if layer == 0:
            own_turn(1)
        for kind in SECOND:
            input_copy(layer, 0, kind, True).wait_recv()
        relay(layer, 2, 0)
        for kind in ONWARD:
            input_copy(layer, 1, kind, True).wait_recv()
        pair_inputs(layer).start()
        if layer == 0:
            for load in loads[2:]:
                load.wait()
        multiply_far(layer, 0)
        for piece in range(1, PIECES):
            relay(layer, 2, piece)
        if layer == 0:
            own_turn(2)
            send_own_core(1)
        multiply_far(layer, 1)
        for piece in range(PIECES):
            relay(layer, 3, piece)
        multiply_far(layer, 2)
        multiply_far(layer, 3)
        for part in (0, 1):
            finish(layer, part)
            if layer + 1 < layers:
                for kind in FIRST + SECOND:
                    if kind[1] == part:
                        input_copy(layer + 1, 0, kind).start()
        if layer == 0:
            @pl.when(place.outer)
            def _():
                ship_copy(0).start()
                ship_copy(1).start()
            drain_weights(0)

    @pl.when(place.inner)
    def _():
        ship_copy(0).wait_recv()
        ship_copy(1).wait_recv()
        stage_copy().start()
        stage_copy(True).wait_recv()
        for kind in FIRST + SECOND:
            spread_copy(0, kind).start()
        for kind in FIRST:
            spread_copy(0, kind, True).wait_recv()
        for kind in ONWARD:
            spread_copy(1, kind).start()
        for kind in SECOND:
            spread_copy(0, kind, True).wait_recv()
        for kind in ONWARD:
            spread_copy(1, kind, True).wait_recv()

    planes = place.planes
    bhalf = learner_rows // 2
    bf16, f32 = jnp.bfloat16, jnp.float32
    top = layers - 1
    own_rows = pl.ds(pl.multiple_of(core * learner_rows, learner_rows), learner_rows)
    other_rows = pl.ds(pl.multiple_of((1 - core) * learner_rows, learner_rows), learner_rows)
    slot_width = width // (2 * planes)

    def pair_grads(layer, arriving=False):
        span = pair_grad.at[layer, other_rows if arriving else own_rows]
        return remote(span, span, p_sent.at[1, layer], p_landed.at[1, layer], place.to_core)

    def head_swap(arriving=False):
        return remote(head_pair.at[0], head_pair.at[1], h_sent.at[2], h_landed.at[2],
                      place.to_core)


    def small(stage, peer):
        return remote(head_send.at[stage], head_land.at[stage], h_sent.at[stage],
                      h_landed.at[stage], peer)

    outputs_used = head_raw.shape[0]
    partial_head = lax.dot_general(
        head_weights[...], last_buf[...], (((1,), (1,)), ((), ())), preferred_element_type=f32)
    for stage, peer in enumerate((place.to_x, place.to_y)):
        head_send[stage] = partial_head
        small(stage, peer).start()
        small(stage, peer).wait_recv()
        partial_head = head_send[stage] + head_land[stage]
    head_send[2] = partial_head
    actor_result[...] = head_send[2, pl.ds(0, outputs_used - 1), pl.ds(learner_rows, rows - learner_rows)]
    actor_copy = pltpu.make_async_copy(actor_result, actor_out, out_sem.at[0, PIECES])
    actor_copy.start()
    learner_head = head_send[2, :, :learner_rows]
    gradient = trace_columns(learner_head, packed[...], outputs_used - 1).astype(bf16)
    rows_each = learner_rows // 4
    for part in range(4):
        span = pl.ds(part * rows_each, rows_each)
        column = lax.dot_general(
            gradient[:, part * rows_each:(part + 1) * rows_each], head_weights[...],
            (((0,), (0,)), ((), ())), preferred_element_type=f32)
        value = total[top, span, :]
        sigma = jax.nn.sigmoid(value)
        slope = sigma * (1.0 + value * (1.0 - sigma))
        pair_grad[top, pl.ds(pl.multiple_of(core * learner_rows + part * rows_each, rows_each), rows_each), :] = (
            column * slope).astype(bf16)
    pair_grads(top).start()
    head_pair[0] = lax.dot_general(
        gradient, last_buf[pl.ds(0, learner_rows), :], (((1,), (0,)), ((), ())),
        preferred_element_type=f32)
    head_swap().start()

    lanes = ((place.to_x, place.to_y), (place.to_y, place.to_x))
    near = ((place.near_x, place.near_y), (place.near_y, place.near_x))
    far_quarter = (place.near_x + 2) % 4

    def first_copy(part, slot):
        span = pl.ds(slot * bhalf, bhalf)
        return remote(weight_buf.at[0, part, span], weight_buf.at[0, 2 + part, span], f_sent.at[0, part, slot],
                      f_landed.at[0, part, slot], lanes[part][0])

    def second_copy(part):
        span = pl.ds(part * bhalf, bhalf)
        return remote(weight_buf.at[0, 4, span], weight_buf.at[0, 5, span], f_sent.at[1, part, 0],
                      f_landed.at[1, part, 0], lanes[part][1])

    def input_quarter(quarter, rows_of):
        parts = []
        for block in range(2):
            parts.append(lax.dot_general(
                pair_grad[top, rows_of, :], weight_buf[top, 2 * quarter + block],
                (((1,), (1,)), ((), ())), preferred_element_type=f32))
        return parts

    cores = pl.multiple_of(core * learner_rows, learner_rows)

    def rows_at(part):
        return pl.ds(pl.multiple_of(cores + part * bhalf, bhalf), bhalf)

    def block_cols(block):
        return pl.ds(block * in_block, in_block)

    def send_first(part, slot, quarter):
        for block, value in enumerate(input_quarter(quarter, rows_at(part))):
            weight_buf[0, part, pl.ds(slot * bhalf, bhalf), block_cols(block)] = value.astype(bf16)
        first_copy(part, slot).start()

    def keep_quarter(part, slot, quarter):
        for block, value in enumerate(input_quarter(quarter, rows_at(part))):
            keep[part, slot, :, block_cols(block)] = value

    def order(step):
        table = []
        for at in range(planes):
            up = list(range(planes - 1, at, -1))
            down = list(range(0, at))
            mixed = []
            while up or down:
                if up:
                    mixed.append(up.pop(0))
                if down:
                    mixed.append(down.pop(0))
            table.append((mixed + [at])[step])
        plane = table[-1]
        for at in range(planes - 1):
            plane = jnp.where(z == at, table[at], plane)
        return plane

    def top_order(step):
        low = (planes - 1, planes // 2, 0)[step]
        high = (0, planes // 2 - 1, planes - 1)[step]
        return jnp.where(z < planes // 2, low, high)

    def line_send(layer, plane, piece, way):
        source = line.at[layer, plane, pl.ds(piece * piece_rows, piece_rows)]
        if way == 0:
            slot = plane
        else:
            slot = jnp.where(plane == z - 1, planes, plane)
        target = line.at[layer, slot, pl.ds(piece * piece_rows, piece_rows)]
        return remote(source, target, lz_sent.at[layer, plane, piece],
                      lz_landed.at[layer, slot, piece], place.to_way[way])

    def line_arrival(layer, slot, piece):
        span = line.at[layer, slot, pl.ds(piece * piece_rows, piece_rows)]
        return remote(span, span, lz_sent.at[layer, 0, piece],
                      lz_landed.at[layer, slot, piece], place.to_core)

    def product(layer, plane, piece, columns):
        contract = (((0,), (0,)), ((), ()))
        mine = pl.ds(pl.multiple_of(core * in_block + piece * piece_rows, piece_rows), piece_rows)
        value = lax.dot_general(
            input_buf[layer, plane, pl.ds(0, learner_rows), mine],
            pair_grad[layer, own_rows, columns], contract, preferred_element_type=f32)
        value = value + lax.dot_general(
            pair_in[layer, plane, :, pl.ds(piece * piece_rows, piece_rows)],
            pair_grad[layer, other_rows, columns], contract, preferred_element_type=f32)
        if layer == top:
            for owner in range(2):
                value = value + lax.dot_general(
                    ship[plane, owner_rows[owner], pl.ds(piece * piece_rows, piece_rows)],
                    weight_buf[0, 6 + owner, :, columns], contract, preferred_element_type=f32)
        return value

    tile = PRODUCT_TILE
    tiles = width // tile

    def over_tiles(body):
        def step(index, carry):
            body(pl.ds(pl.multiple_of(index * tile, tile), tile))
            return carry
        lax.fori_loop(0, tiles, step, 0)

    def pass_on(layer, step):
        if layer == top:
            plane = top_order(step)
            upward = plane > z
            fed = plane == place.mate
        else:
            plane = order(step)
            upward = plane > z
            fed = jnp.where(upward, z > 0, z + 1 < planes)
        for piece in range(PIECES):
            span = pl.ds(piece * piece_rows, piece_rows)

            @pl.when(fed)
            def _():
                line_arrival(layer, plane, piece).wait_recv()

                def body(columns):
                    value = product(layer, plane, piece, columns)
                    value = value + line[layer, plane, span, columns].astype(f32)
                    line[layer, plane, span, columns] = value.astype(bf16)
                over_tiles(body)

            @pl.when(jnp.logical_not(fed))
            def _():
                def body(columns):
                    value = product(layer, plane, piece, columns)
                    line[layer, plane, span, columns] = value.astype(bf16)
                over_tiles(body)

            pl.when(upward)(line_send(layer, plane, piece, 0).start)
            pl.when(jnp.logical_not(upward))(line_send(layer, plane, piece, 1).start)

    def head_line(plane, way, receiving):
        slot = plane
        if way == 1 and not receiving:
            slot = jnp.where(plane == z - 1, planes, plane)
        return remote(head_sum.at[plane], head_sum.at[slot], hl_sent.at[plane],
                      hl_landed.at[slot], place.to_core if receiving else place.to_way[way])

    def head_columns(which, plane):
        start = pl.multiple_of((2 * plane + core) * slot_width, slot_width)
        return head_pair[which, :, pl.ds(start, slot_width)]

    def head_pass(step):
        plane = order(step)
        upward = plane > z
        fed = jnp.where(upward, z > 0, z + 1 < planes)
        own = head_columns(0, plane) + head_columns(1, plane)

        @pl.when(fed)
        def _():
            head_line(plane, 0, True).wait_recv()
            head_sum[plane] = head_sum[plane] + own

        @pl.when(jnp.logical_not(fed))
        def _():
            head_sum[plane] = own

        pl.when(upward)(head_line(plane, 0, False).start)
        pl.when(jnp.logical_not(upward))(head_line(plane, 1, False).start)

    def head_final():
        head_land[0, :, pl.ds(0, slot_width)] = head_columns(0, z) + head_columns(1, z)
        for slot, present in ((z, z > 0), (planes, z + 1 < planes)):
            @pl.when(present)
            def _():
                head_line(slot, 0, True).wait_recv()
                head_land[0, :, pl.ds(0, slot_width)] += head_sum[slot]
        head_result[...] = head_land[0, pl.ds(0, outputs_used), pl.ds(0, slot_width)]
        pltpu.make_async_copy(head_result, head_grads_out, out_sem.at[1, PIECES]).start()

    def drain(layer, step):
        plane = top_order(step) if layer == top else order(step)
        for piece in range(PIECES):
            span = line.at[layer, plane, pl.ds(piece * piece_rows, piece_rows)]
            remote(span, span, lz_sent.at[layer, plane, piece],
                   lz_landed.at[layer, plane, piece], place.to_core).wait_send()

    def own_product(layer):
        for piece in range(PIECES):
            span = pl.ds(piece * piece_rows, piece_rows)

            def body(columns):
                total[layer, span, columns] = product(layer, z, piece, columns)
            over_tiles(body)

    def own_add(layer):
        for piece in range(PIECES):
            span = pl.ds(piece * piece_rows, piece_rows)
            if layer == top:
                cases = ((z, z >= planes // 2), (planes, z < planes // 2))
            else:
                cases = ((z, z > 0), (planes, z + 1 < planes))
            for slot, present in cases:
                @pl.when(present)
                def _():
                    line_arrival(layer, slot, piece).wait_recv()
                    total[layer, span, :] += line[layer, slot, span, :].astype(f32)
            pltpu.make_async_copy(
                total.at[layer, span], grads_out.at[layer, span],
                out_sem.at[layer, piece]).start()


    @pl.when(place.outer)
    def _():
        for piece in range(2):
            grad_ship(piece).start()
    for part in range(2):
        send_first(part, 0, far_quarter)
    for part in range(2):
        send_first(part, 1, near[part][0])
    for part in range(2):
        keep_quarter(part, 1, near[part][1])
        keep_quarter(part, 0, group)
    head_swap(True).wait_recv()
    head_pass(0)
    pair_grads(top, True).wait_recv()
    pair_inputs(top).wait_recv()
    for part in range(2):
        first_copy(part, 0).wait_recv()
        weight_buf[0, 4, pl.ds(part * bhalf, bhalf), :] = (
            keep[part, 1] + weight_buf[0, 2 + part, pl.ds(0, bhalf), :].astype(f32)).astype(bf16)
        second_copy(part).start()

    @pl.when(place.inner)
    def _():
        for piece in range(2):
            grad_ship(piece).wait_recv()
            grad_swap(piece).start()
        for piece in range(2):
            grad_swap(piece, True).wait_recv()
        pass_on(top, 0)
    for part in range(2):
        first_copy(part, 1).wait_recv()
        second_copy(part).wait_recv()
        summed = keep[part, 0] + weight_buf[0, 2 + part, pl.ds(bhalf, bhalf), :].astype(f32)
        summed = summed + weight_buf[0, 5, pl.ds(part * bhalf, bhalf), :].astype(f32)
        value = total[0, pl.ds(part * bhalf, bhalf), :]
        sigma = jax.nn.sigmoid(value)
        slope = sigma * (1.0 + value * (1.0 - sigma))
        pair_grad[0, rows_at(part), :] = (summed * slope).astype(bf16)
    pair_grads(0).start()
    pl.when(place.inner)(functools.partial(pass_on, top, 1))
    pair_grads(0, True).wait_recv()
    pair_inputs(0).wait_recv()
    pass_on(0, 0)
    head_pass(1)
    head_pass(2)
    pass_on(0, 1)

    @pl.when(place.inner)
    def _():
        pass_on(top, 2)
        own_product(top)

    @pl.when(place.outer)
    def _():
        total[top, pl.ds(0, learner_rows), :] = jnp.zeros((learner_rows, width), f32)
    pass_on(0, 2)
    own_product(0)
    own_add(top)
    head_final()
    own_add(0)

    for layer in range(layers):
        pair_inputs(layer).wait_send()
        pair_grads(layer).wait_send()
        for step in range(planes - 1):
            if layer == top:
                pl.when(place.inner)(functools.partial(drain, layer, step))
            else:
                drain(layer, step)
        for piece in range(PIECES):
            span = pl.ds(piece * piece_rows, piece_rows)
            pltpu.make_async_copy(
                total.at[layer, span], grads_out.at[layer, span],
                out_sem.at[layer, piece]).wait()
    for part in range(2):
        for slot in range(2):
            first_copy(part, slot).wait_send()
        second_copy(part).wait_send()
    small(0, place.to_x).wait_send()
    small(1, place.to_y).wait_send()
    head_swap().wait_send()
    for step in range(planes - 1):
        head_line(order(step), 0, True).wait_send()
    actor_copy.wait()
    pltpu.make_async_copy(head_result, head_grads_out, out_sem.at[1, PIECES]).wait()

    for layer in range(layers):
        for kind in FIRST + SECOND:
            input_copy(layer, 0, kind).wait_send()
        for kind in ONWARD:
            input_copy(layer, 1, kind).wait_send()
    for layer in range(1, layers):
        drain_weights(layer)

    @pl.when(place.outer)
    def _():
        for other in range(2):
            ship_copy(other).wait_send()
            grad_ship(other).wait_send()

    @pl.when(place.inner)
    def _():
        stage_copy().wait_send()
        for kind in FIRST + SECOND:
            spread_copy(0, kind).wait_send()
        for kind in ONWARD:
            spread_copy(1, kind).wait_send()
        for piece in range(2):
            grad_swap(piece).wait_send()


def trace_columns(outputs, packed, actions_total):
    count, columns = outputs.shape
    row = lax.broadcasted_iota(jnp.int32, (count, columns), 0)
    is_action = row < actions_total
    behave, action = packed[0:1], packed[1:2]
    rewards, finished, live = packed[2:3], packed[3:4], packed[4:5]

    def after(value, reach):
        return pltpu.roll(value, columns - reach, 1)

    peak = jnp.max(jnp.where(is_action, outputs, -jnp.inf), axis=0, keepdims=True)
    shifted = jnp.where(is_action, outputs - peak, 0.0)
    weight = jnp.where(is_action, jnp.exp(shifted), 0.0)
    scale = jnp.sum(weight, axis=0, keepdims=True)
    log_policy = jnp.where(is_action, shifted - jnp.log(scale), 0.0)
    probability = jnp.where(is_action, jnp.exp(log_policy), 0.0)
    chosen = jnp.where(row == action.astype(jnp.int32), 1.0, 0.0)
    ratio = jnp.exp(jnp.sum(log_policy * chosen, axis=0, keepdims=True) - behave)
    clipped = jnp.minimum(ratio, 1.0)
    discount = discount_rate * (1.0 - finished)
    current = jnp.sum(jnp.where(row == actions_total, outputs, 0.0), axis=0, keepdims=True)
    corrections = live * clipped * (rewards + discount * after(current, 1) - current)
    factors = live * discount * clipped
    reach = 1
    while reach < columns:
        corrections = corrections + factors * after(corrections, reach)
        factors = factors * after(factors, reach)
        reach *= 2
    targets = current + corrections
    advantage = clipped * (rewards + discount * after(targets, 1) - current)
    entropy = -jnp.sum(probability * log_policy, axis=0, keepdims=True)
    logit_grad = (
        -advantage * (chosen - probability)
        + entropy_weight * probability * (log_policy + entropy)
    ) / loss_divisor
    value_grad = -value_weight * (targets - current) / loss_divisor
    result = jnp.where(is_action, logit_grad, jnp.where(row == actions_total, value_grad, 0.0))
    return jnp.where(live > 0.0, result, 0.0)


def exact_dot(left, right, dims):
    return lax.dot_general(
        left, right, (dims, ((), ())), precision=lax.Precision.HIGHEST,
        preferred_element_type=jnp.float32)


def prepare(head_own, acting_own, actions_own, rewards_own, finished_own, head_weights, packed):
    padded, used = head_weights.shape[0], head_own.shape[0]
    row = lax.broadcasted_iota(jnp.int32, (padded, used), 0)
    column = lax.broadcasted_iota(jnp.int32, (padded, used), 1)
    select = jnp.where(row == column, 1.0, 0.0).astype(jnp.bfloat16)
    head_weights[...] = lax.dot_general(
        select, head_own[...], (((1,), (0,)), ((), ())), preferred_element_type=jnp.float32
    ).astype(jnp.bfloat16)
    actions_total, trajectories, steps = acting_own.shape
    columns = packed.shape[1]
    span = columns // trajectories
    step = lax.broadcasted_iota(jnp.int32, (steps, columns), 0)
    place = lax.broadcasted_iota(jnp.int32, (steps, columns), 1)
    spread = jnp.where(place % span == step, 1.0, 0.0)
    owner = lax.broadcasted_iota(jnp.int32, (trajectories, columns), 0)
    where = lax.broadcasted_iota(jnp.int32, (trajectories, columns), 1)
    mine = where // span == owner

    def flat(array):
        wide = exact_dot(array.astype(jnp.float32), spread, ((1,), (0,)))
        return jnp.sum(jnp.where(mine, wide, 0.0), axis=0, keepdims=True)

    action = flat(actions_own[...])
    scores = jnp.concatenate([flat(acting_own[at]) for at in range(actions_total)], axis=0)
    peak = jnp.max(scores, axis=0, keepdims=True)
    shifted = scores - peak
    scale = jnp.sum(jnp.exp(shifted), axis=0, keepdims=True)
    kind = lax.broadcasted_iota(jnp.int32, (actions_total, columns), 0)
    taken = jnp.sum(jnp.where(kind == action.astype(jnp.int32), shifted, 0.0), axis=0, keepdims=True)
    packed[0:1, :] = taken - jnp.log(scale)
    packed[1:2, :] = action
    packed[2:3, :] = flat(rewards_own[...])
    packed[3:4, :] = flat(finished_own[...])
    live = lax.broadcasted_iota(jnp.int32, (1, columns), 1) % span < steps
    packed[4:5, :] = jnp.where(live, 1.0, 0.0)


def whole_step(observations, next_observations, weights, head_weights, acting, *per_step):
    layers, in_block, width = weights.shape
    learner_rows = observations.shape[0]
    rows = learner_rows + next_observations.shape[0]
    used = head_weights.shape[0]
    padded = -(-used // 16) * 16
    planes = lax.axis_size("dp") // 2
    bf16, f32 = jnp.bfloat16, jnp.float32
    half = learner_rows // 2
    dma = pltpu.SemaphoreType.DMA
    hbm = pl.BlockSpec(memory_space=pltpu.HBM)
    slot_width = width // (2 * planes)
    return pl.pallas_call(
        step_kernel,
        out_shape=(
            jax.ShapeDtypeStruct((layers, in_block, width), f32),
            jax.ShapeDtypeStruct((used, slot_width), f32),
            jax.ShapeDtypeStruct((used - 1, rows - learner_rows), f32),
        ),
        in_specs=[hbm] * 8,
        out_specs=(hbm,) * 3,
        scratch_shapes=[
            pltpu.VMEM((layers, 2 * planes, in_block, width), bf16),
            pltpu.VMEM((layers, 4, rows, width), bf16),
            pltpu.VMEM((rows, width), bf16),
            pltpu.VMEM((layers, rows, width), f32),
            pltpu.VMEM((layers, 4, learner_rows, in_block), bf16),
            pltpu.VMEM((layers, 2 * learner_rows, width), bf16),
            pltpu.VMEM((layers, planes + 1, in_block, width), bf16),
            pltpu.VMEM((2, 2, half, width), f32),
            pltpu.VMEM((4, 2 * learner_rows, in_block), bf16),
            pltpu.VMEM((learner_rows, in_block), bf16),
            pltpu.VMEM((3, padded, rows), f32),
            pltpu.VMEM((2, padded, rows), f32),
            pltpu.VMEM((2, padded, width), f32),
            pltpu.VMEM((planes + 1, padded, slot_width), f32),
            pltpu.VMEM(head_weights.shape, bf16),
            pltpu.VMEM(acting.shape, f32),
        ] + [pltpu.VMEM(array.shape, array.dtype) for array in per_step] + [
            pltpu.VMEM((padded, width), bf16),
            pltpu.VMEM((8, learner_rows), f32),
            pltpu.VMEM((used, slot_width), f32),
            pltpu.VMEM((used - 1, rows - learner_rows), f32),
            dma((7 + layers,)),
            dma((layers, 2, 2, 2)), dma((layers, 2, 2, 2)),
            dma((layers, 2, 4, PIECES)), dma((layers, 2, 4, PIECES)),
            dma((layers, 2, 4, PIECES)), dma((layers, 2, 4, PIECES)),
            dma((2, layers)), dma((2, layers)),
            dma((layers, planes + 1, PIECES)), dma((layers, planes + 1, PIECES)),
            dma((2, 2, 2)), dma((2, 2, 2)),
            dma((3,)), dma((3,)),
            dma((planes + 1,)), dma((planes + 1,)),
            dma((16,)), dma((16,)),
            dma((layers, PIECES + 1)),
        ],
        compiler_params=pltpu.CompilerParams(
            collective_id=0, has_side_effects=True, vmem_limit_bytes=VMEM_LIMIT),
        name="learner_step",
    )(observations, next_observations, weights, head_weights, acting, *per_step)


def per_device_line(
    observations, next_observations, trunk_weights, head_weights,
    acting_policy_logits, actions, rewards, episode_finished,
):
    traj_count, step_count, feature_block = observations.shape
    learner_rows = traj_count * step_count
    trunk_grads, head_grads, actor_logits = whole_step(
        observations.reshape(learner_rows, feature_block), next_observations, trunk_weights,
        head_weights.T, acting_policy_logits.transpose(2, 0, 1), actions, rewards,
        episode_finished)
    return trunk_grads, head_grads.T, actor_logits.T


def solution(mesh):
    in_specs = (
        P("dp", None, "group"),
        P("dp", "group"),
        P(None, "dp", "group"),
        P("group", None),
        P("dp", None, None),
        P("dp", None),
        P("dp", None),
        P("dp", None),
    )
    out_specs = (P(None, "dp", "group"), P(("group", "dp"), None), P("dp", None))
    body = functools.partial(per_device, mesh.shape["group"], mesh.shape["dp"])
    if (mesh.shape["group"], mesh.shape["dp"]) == (4, 8):
        body = per_device_line
    return jax.shard_map(
        body, mesh=mesh, in_specs=in_specs, out_specs=out_specs, check_vma=False
    )
```

```python
import functools

import jax
import jax.numpy as jnp
from jax import lax
from jax.experimental import pallas as pl
from jax.experimental.pallas import tpu as pltpu
from jax.sharding import PartitionSpec as P

discount_rate = 0.99
value_weight = 0.5
entropy_weight = 0.1
loss_divisor = 16.0


def contract_rows(left, right):
    return lax.dot_general(
        left, right, (((0,), (0,)), ((), ())), preferred_element_type=jnp.float32
    )


def contract_cols(left, right):
    return lax.dot_general(
        left, right, (((1,), (1,)), ((), ())), preferred_element_type=jnp.float32
    )


def silu_slope(pre_value):
    sigma = jax.nn.sigmoid(pre_value)
    return sigma * (1.0 + pre_value * (1.0 - sigma))


def importance_trace_gradients(
    learner_output, acting_policy_logits, actions, rewards, episode_finished
):
    log_behave = jax.nn.log_softmax(acting_policy_logits, axis=-1)
    chosen = actions[:, :, None] == jnp.arange(log_behave.shape[-1], dtype=jnp.int32)
    behave = jnp.sum(jnp.where(chosen, log_behave, 0.0), axis=-1)
    return trace_gradients(
        learner_output, behave, actions, rewards, episode_finished.astype(jnp.float32)
    )


def trace_gradients_packed(learner_output, packed):
    behave, actions, rewards, finished = packed
    return trace_gradients(learner_output, behave, actions.astype(jnp.int32), rewards, finished)


def trace_gradients(learner_output, behave, actions, rewards, finished):
    number_of_actions = learner_output.shape[-1] - 1
    logits = learner_output[:, :, :number_of_actions]
    values = learner_output[:, :, number_of_actions]
    log_policy = jax.nn.log_softmax(logits[:, :-1], axis=-1)
    chosen = (
        actions[:, :, None] == jnp.arange(number_of_actions, dtype=jnp.int32)[None, None, :]
    ).astype(jnp.float32)
    ratio = jnp.exp(jnp.sum(log_policy * chosen, axis=-1) - behave)
    clipped = jnp.minimum(ratio, 1.0)
    discount = discount_rate * (1.0 - finished)
    current = values[:, :-1]
    following = values[:, 1:]
    deltas = clipped * (rewards + discount * following - current)

    corrections, factors = deltas, discount * clipped
    reach, span = 1, deltas.shape[1]
    while reach < span:
        later = jnp.pad(corrections[:, reach:], ((0, 0), (0, reach)))
        later_factors = jnp.pad(factors[:, reach:], ((0, 0), (0, reach)))
        corrections = corrections + factors * later
        factors = factors * later_factors
        reach *= 2
    targets = current + corrections
    next_targets = jnp.concatenate([targets[:, 1:], values[:, -1:]], axis=1)
    advantage = clipped * (rewards + discount * next_targets - current)
    probability = jnp.exp(log_policy)
    entropy = -jnp.sum(probability * log_policy, axis=-1)
    logit_grad = (
        -advantage[..., None] * (chosen - probability)
        + entropy_weight * probability * (log_policy + entropy[..., None])
    ) / loss_divisor
    value_grad = -value_weight * (targets - current) / loss_divisor
    step_grad = jnp.concatenate([logit_grad, value_grad[..., None]], axis=-1)
    last_row = jnp.zeros((values.shape[0], 1, number_of_actions + 1), jnp.float32)
    return jnp.concatenate([step_grad, last_row], axis=1)


def swap(block, mask, size):
    return lax.ppermute(block, "group", [(index, index ^ mask) for index in range(size)])


def gather_features(block, size):
    if size != 4:
        return lax.all_gather(block, "group", axis=1, tiled=True)
    me = lax.axis_index("group")
    rows, width = block.shape
    half = rows // 2
    from_near = swap(block, 1, size)
    from_far = swap(block, 2, size)
    top = swap(from_near[:half], 2, size)
    bottom = swap(from_far[half:], 1, size)
    whole = jnp.zeros((rows, size * width), block.dtype)
    whole = lax.dynamic_update_slice(whole, block, (0, me * width))
    whole = lax.dynamic_update_slice(whole, from_near, (0, (me ^ 1) * width))
    whole = lax.dynamic_update_slice(whole, from_far, (0, (me ^ 2) * width))
    whole = lax.dynamic_update_slice(whole, top, (0, (me ^ 3) * width))
    return lax.dynamic_update_slice(whole, bottom, (half, (me ^ 3) * width))


def scatter_features(partial, size):
    if size != 4:
        return lax.psum_scatter(partial, "group", scatter_dimension=1, tiled=True)
    me = lax.axis_index("group")
    rows, width = partial.shape[0], partial.shape[1] // size
    half = rows // 2
    wire = jnp.bfloat16

    def part(start, mask):
        piece = lax.dynamic_slice(partial, (start, (me ^ mask) * width), (half, width))
        return piece

    def reduce_half(start, first, second):
        theirs = jnp.concatenate([part(start, first), part(start, 3)], axis=0)
        got = swap(theirs, first, size)
        onward = part(start, second).astype(jnp.float32) + got[half:].astype(jnp.float32)
        mine = part(start, 0).astype(jnp.float32) + got[:half].astype(jnp.float32)
        return mine + swap(onward.astype(wire), second, size).astype(jnp.float32)

    return jnp.concatenate([reduce_half(0, 1, 2), reduce_half(half, 2, 1)], axis=0)


def scatter_rows(block, size):
    if size & (size - 1):
        return lax.psum_scatter(block, "dp", scatter_dimension=0, tiled=True)
    me = lax.axis_index("dp")
    mask = size // 2
    while mask:
        half = block.shape[0] // 2
        upper = (me & mask) > 0
        theirs = jnp.where(upper, block[:half], block[half:])
        mine = jnp.where(upper, block[half:], block[:half])
        block = mine + lax.ppermute(theirs, "dp", [(i, i ^ mask) for i in range(size)])
        mask //= 2
    return block


def swap_cores(block, size):
    return lax.ppermute(block, "dp", [(index, index ^ 1) for index in range(size)])


def split_for_pair(whole, size):
    core = lax.axis_index("dp") % 2
    rows, width = whole.shape
    by_owner = whole.reshape(rows, size // 2, 2, width // size)

    def features_of(owner):
        picked = lax.dynamic_slice_in_dim(by_owner, owner, 1, axis=2)
        return picked.reshape(rows, width // 2)

    return features_of(core), swap_cores(features_of(1 - core), size)


def sum_group(block, size):
    if size != 4:
        return lax.psum(block, "group")
    block = block + swap(block, 1, size)
    return block + swap(block, 2, size)


def per_device(
    group_size,
    dp_size,
    observations,
    next_observations,
    trunk_weights,
    head_weights,
    acting_policy_logits,
    actions,
    rewards,
    episode_finished,
):
    traj_count, step_count, feature_block = observations.shape
    learner_rows = traj_count * step_count
    number_of_actions = acting_policy_logits.shape[-1]
    layer_total = trunk_weights.shape[0]
    own_rows = observations.reshape(learner_rows, feature_block)
    gathered_weights = [
        lax.all_gather(trunk_weights[layer_index], "dp", axis=0, tiled=True)
        for layer_index in range(layer_total)
    ]
    current = jnp.concatenate([own_rows, next_observations], axis=0)
    pair_inputs = []
    products_block = []
    for layer_index in range(layer_total):
        whole = gather_features(current, group_size)
        product = jnp.dot(
            whole, gathered_weights[layer_index], preferred_element_type=jnp.float32
        )
        pair_inputs.append(split_for_pair(whole[:learner_rows], dp_size))
        products_block.append(product[:learner_rows])
        current = jax.nn.silu(product).astype(jnp.bfloat16)
    partial_head = jnp.dot(current, head_weights, preferred_element_type=jnp.float32)
    totals = sum_group(partial_head, group_size)
    last_block = current[:learner_rows]
    head_out = totals[:learner_rows]
    actor_logits = totals[learner_rows:, :number_of_actions]
    learner_output = head_out.reshape(traj_count, step_count, number_of_actions + 1)
    output_gradient = importance_trace_gradients(
        learner_output, acting_policy_logits, actions, rewards, episode_finished
    )
    output_gradient = output_gradient.reshape(learner_rows, number_of_actions + 1).astype(
        jnp.bfloat16
    )
    input_grad = contract_cols(output_gradient, head_weights)
    grad_list = [None] * layer_total
    for layer_index in range(layer_total - 1, -1, -1):
        pre_grad = (input_grad * silu_slope(products_block[layer_index])).astype(jnp.bfloat16)
        near_inputs, far_inputs = pair_inputs[layer_index]
        far_grad = swap_cores(pre_grad, dp_size)
        partial = contract_rows(near_inputs, pre_grad) + contract_rows(far_inputs, far_grad)
        partial = partial.astype(jnp.bfloat16)
        partial, pre_grad = lax.optimization_barrier((partial, pre_grad))
        grad_list[layer_index] = lax.psum_scatter(
            partial,
            "dp",
            scatter_dimension=0,
            tiled=True,
            axis_index_groups=[list(range(core, dp_size, 2)) for core in range(2)],
        ).astype(jnp.float32)
        if layer_index > 0:
            full_grad = contract_cols(pre_grad, gathered_weights[layer_index]).astype(jnp.bfloat16)
            input_grad = scatter_features(full_grad, group_size)
    head_partial = contract_rows(last_block, output_gradient)
    head_grads = scatter_rows(head_partial, dp_size)
    return (jnp.stack(grad_list), head_grads, actor_logits)


MESH = pl.DeviceIdType.MESH
PIECES = 2
TILE = 256
PRODUCT_TILE = 512
VMEM_LIMIT = 67043328


class Place:
    def __init__(self):
        group, dp = lax.axis_index("group"), lax.axis_index("dp")
        self.group, self.dp = group, dp
        self.x, self.core, self.z = group % 2, dp % 2, dp // 2
        self.near_x = group + 1 - 2 * self.x
        self.near_y = (group + 2) % 4
        self.planes = lax.axis_size("dp") // 2
        self.to_x = (self.near_x, dp)
        self.to_y = (self.near_y, dp)
        self.to_core = (group, dp + 1 - 2 * self.core)
        self.to_way = ((group, dp + 2), (group, dp - 2))
        self.mate = self.z + 1 - 2 * (self.z % 2)
        self.to_mate = (group, 2 * self.mate + self.core)
        self.outer = jnp.logical_or(self.z == 0, self.z == self.planes - 1)
        self.inner = jnp.logical_not(self.outer)

    def source(self, way, far):
        return self.z - far if way == 0 else self.z + far

    def has_source(self, way, far):
        return self.z >= far if way == 0 else self.z + far < self.planes

    def has_next(self, way):
        return self.z + 1 < self.planes if way == 0 else self.z > 0

    def greet(self):
        barrier = pltpu.get_barrier_semaphore()
        for peer in (self.to_x, self.to_y, self.to_core):
            pl.semaphore_signal(barrier, inc=1, device_id=peer, device_id_type=MESH)
        for way in range(2):
            @pl.when(self.has_next(way))
            def _():
                pl.semaphore_signal(
                    barrier, inc=1, device_id=self.to_way[way], device_id_type=MESH)
        inner = jnp.logical_and(self.has_next(0), self.has_next(1))
        pl.semaphore_wait(barrier, jnp.where(inner, 5, 4))


def remote(source, target, sent, landed, peer):
    return pltpu.make_async_remote_copy(
        src_ref=source, dst_ref=target, send_sem=sent, recv_sem=landed,
        device_id=peer, device_id_type=MESH)


def step_kernel(
    observations, next_observations, weights, head_raw, acting_raw, actions_raw, rewards_raw,
    finished_raw, grads_out, head_grads_out, actor_out,
    weight_buf, input_buf, last_buf, total, pair_in, pair_grad, line, keep, ship, stage, head_send, head_land, head_pair, head_sum, head_own, acting_own,
    actions_own, rewards_own, finished_own, head_weights, packed, head_result, actor_result,
    local_sem, x_sent, x_landed, z_sent, z_landed, c_sent, c_landed, p_sent, p_landed,
    lz_sent, lz_landed, f_sent, f_landed, h_sent, h_landed, hl_sent, hl_landed, s_sent, s_landed, out_sem,
):
    place = Place()
    group, dp, z, core = place.group, place.dp, place.z, place.core
    layers, in_block, width = weights.shape
    learner_rows = observations.shape[0]
    rows = learner_rows + next_observations.shape[0]
    half = rows // 2
    piece_rows = in_block // PIECES
    halves = (pl.ds(0, half), pl.ds(half, half))

    loads = [
        pltpu.make_async_copy(
            observations, input_buf.at[0, group, pl.ds(0, learner_rows)], local_sem.at[0]),
        pltpu.make_async_copy(
            next_observations,
            input_buf.at[0, group, pl.ds(learner_rows, rows - learner_rows)], local_sem.at[1]),
    ] + [
        pltpu.make_async_copy(weights.at[layer], weight_buf.at[layer, dp], local_sem.at[2 + layer])
        for layer in range(layers)
    ]

    def weight_copy(layer, way, far, piece):
        block = 2 * place.source(way, far) + core
        span = weight_buf.at[layer, block, pl.ds(piece * piece_rows, piece_rows)]
        source = weights.at[layer, pl.ds(piece * piece_rows, piece_rows)] if far == 0 else span
        return remote(source, span, z_sent.at[layer, way, far, piece],
                      z_landed.at[layer, way, far, piece], place.to_way[way])

    def weight_arrival(layer, way, far, piece):
        block = 2 * place.source(way, far) + core
        span = weight_buf.at[layer, block, pl.ds(piece * piece_rows, piece_rows)]
        return remote(span, span, z_sent.at[layer, way, far - 1, piece],
                      z_landed.at[layer, way, far - 1, piece], place.to_core)

    def core_copy(layer, way, far, piece, arriving=False):
        owner = 1 - core if arriving else core
        block = 2 * place.source(way, far) + owner
        span = weight_buf.at[layer, block, pl.ds(piece * piece_rows, piece_rows)]
        source = span
        if far == 0 and not arriving:
            source = weights.at[layer, pl.ds(piece * piece_rows, piece_rows)]
        return remote(source, span, c_sent.at[layer, way, far, piece],
                      c_landed.at[layer, way, far, piece], place.to_core)

    def send_own_weights(layer, way):
        for piece in range(PIECES):
            weight_copy(layer, way, 0, piece).start()

    def send_own_core(layer):
        for piece in range(PIECES):
            core_copy(layer, 0, 0, piece).start()

    def own_turn(far):
        for way in range(2):
            edge = z == far if way == 0 else place.planes - 1 - z == far
            @pl.when(jnp.logical_and(edge, place.has_next(way)))
            def _():
                for layer in range(1, layers):
                    send_own_weights(layer, way)

    def relay(layer, far, piece):
        for way in range(2):
            @pl.when(place.has_source(way, far))
            def _():
                weight_arrival(layer, way, far, piece).wait_recv()
                @pl.when(place.has_next(way))
                def _():
                    weight_copy(layer, way, far, piece).start()
                core_copy(layer, way, far, piece).start()

    def input_copy(layer, stage, kind, arriving=False):
        lane, part = kind
        peer = (place.to_x, place.to_y)[lane]
        if stage == 0:
            quarter = (place.near_x, place.near_y)[lane] if arriving else group
        else:
            other = (place.near_y, place.near_x)[lane]
            quarter = (place.near_x + 2) % 4 if arriving else other
        span = input_buf.at[layer, quarter, halves[part]]
        index = (layer, stage, lane, part)
        return remote(span, span, x_sent.at[index], x_landed.at[index], peer)

    FIRST = ((0, 0), (1, 1))
    SECOND = ((0, 1), (1, 0))
    ONWARD = ((1, 0), (0, 1))

    def multiply(layer, plane):
        left = input_buf.at[layer, plane]
        right = weight_buf.at[layer, pl.ds(2 * plane, 2)]

        def step(tile, carry):
            columns = pl.ds(pl.multiple_of(tile * TILE, TILE), TILE)
            total[layer, :, columns] += jnp.dot(
                left[...], right[:, :, columns].reshape(width, TILE),
                preferred_element_type=jnp.float32)
            return carry
        lax.fori_loop(0, width // TILE, step, 0)

    def core_arrivals(layer, far):
        for way in range(2 if far else 1):
            def wait():
                for piece in range(PIECES):
                    core_copy(layer, way, far, piece, arriving=True).wait_recv()
            if far:
                pl.when(place.has_source(way, far))(wait)
            else:
                wait()

    def multiply_far(layer, far):
        core_arrivals(layer, far)
        if far == 0:
            multiply(layer, z)
            return
        for way in range(2):
            @pl.when(place.has_source(way, far))
            def _():
                multiply(layer, place.source(way, far))

    def finish(layer, part):
        span = halves[part]
        value = total[layer, span, :]
        result = (value * jax.nn.sigmoid(value)).astype(jnp.bfloat16)
        if layer + 1 < layers:
            input_buf[layer + 1, group, span, :] = result
        else:
            last_buf[span, :] = result

    other_cols = pl.ds(pl.multiple_of((1 - core) * in_block, in_block), in_block)

    def pair_inputs(layer):
        source = input_buf.at[layer, :, pl.ds(0, learner_rows), other_cols]
        return remote(source, pair_in.at[layer], p_sent.at[0, layer], p_landed.at[0, layer],
                      place.to_core)

    side = [
        pltpu.make_async_copy(source, target, local_sem.at[2 + layers + index])
        for index, (source, target) in enumerate((
            (head_raw, head_own), (acting_raw, acting_own), (actions_raw, actions_own),
            (rewards_raw, rewards_own), (finished_raw, finished_own)))
    ]
    own_cols = pl.ds(pl.multiple_of(core * in_block, in_block), in_block)
    owner_rows = (pl.ds(0, learner_rows), pl.ds(learner_rows, learner_rows))
    core_rows = pl.ds(pl.multiple_of(core * learner_rows, learner_rows), learner_rows)
    mate_rows = pl.ds(pl.multiple_of((1 - core) * learner_rows, learner_rows), learner_rows)

    whole_stage = stage.at[pl.ds(0, learner_rows)]

    def ship_copy(other):
        source = input_buf.at[1, group, pl.ds(0, learner_rows), other_cols if other else own_cols]
        target = whole_stage if other else ship.at[group, core_rows]
        return remote(source, target, s_sent.at[other], s_landed.at[other], place.to_mate)

    def stage_copy(arriving=False):
        return remote(whole_stage, ship.at[group, mate_rows if arriving else core_rows],
                      s_sent.at[2], s_landed.at[2], place.to_core)

    def spread_copy(level, kind, arriving=False):
        lane, part = kind
        peer = (place.to_x, place.to_y)[lane]
        if level == 0:
            quarter = (place.near_x, place.near_y)[lane] if arriving else group
        else:
            other = (place.near_y, place.near_x)[lane]
            quarter = (place.near_x + 2) % 4 if arriving else other
        span = ship.at[quarter, owner_rows[part]]
        index = 3 + level * 4 + lane * 2 + part
        return remote(span, span, s_sent.at[index], s_landed.at[index], peer)

    def grad_ship(piece):
        step = learner_rows // 2
        source = pair_grad.at[layers - 1, pl.ds(
            pl.multiple_of(core * learner_rows + piece * step, step), step)]
        target = weight_buf.at[0, 6 + core, pl.ds(piece * step, step)]
        return remote(source, target, s_sent.at[11 + piece], s_landed.at[11 + piece],
                      place.to_mate)

    def grad_swap(piece, arriving=False):
        step = learner_rows // 2
        owner = 1 - core if arriving else core
        span = weight_buf.at[0, 6 + owner, pl.ds(piece * step, step)]
        return remote(span, span, s_sent.at[13 + piece], s_landed.at[13 + piece], place.to_core)

    def drain_weights(layer):
        for piece in range(PIECES):
            core_copy(layer, 0, 0, piece).wait_send()
            for way in range(2):
                pl.when(place.has_next(way))(weight_copy(layer, way, 0, piece).wait_send)
                for far in (1, 2, 3):
                    @pl.when(place.has_source(way, far))
                    def _():
                        pl.when(place.has_next(way))(
                            weight_copy(layer, way, far, piece).wait_send)
                        core_copy(layer, way, far, piece).wait_send()

    for load in loads + side:
        load.start()
    place.greet()
    for way in range(2):
        pl.when(place.has_next(way))(functools.partial(send_own_weights, 0, way))
    own_turn(0)
    loads[0].wait()
    loads[1].wait()
    for kind in FIRST + SECOND:
        input_copy(0, 0, kind).start()
    send_own_core(0)
    total[...] = jnp.zeros_like(total)
    for copy in side:
        copy.wait()
    prepare(head_own, acting_own, actions_own, rewards_own, finished_own, head_weights, packed)
    for layer in range(layers):
        relay(layer, 1, 0)
        for kind in FIRST:
            input_copy(layer, 0, kind, True).wait_recv()
        for kind in ONWARD:
            input_copy(layer, 1, kind).start()
        for piece in range(1, PIECES):
            relay(layer, 1, piece)
        if layer == 0:
            own_turn(1)
        for kind in SECOND:
            input_copy(layer, 0, kind, True).wait_recv()
        relay(layer, 2, 0)
        for kind in ONWARD:
            input_copy(layer, 1, kind, True).wait_recv()
        pair_inputs(layer).start()
        if layer == 0:
            for load in loads[2:]:
                load.wait()
        multiply_far(layer, 0)
        for piece in range(1, PIECES):
            relay(layer, 2, piece)
        if layer == 0:
            own_turn(2)
            send_own_core(1)
        multiply_far(layer, 1)
        for piece in range(PIECES):
            relay(layer, 3, piece)
        multiply_far(layer, 2)
        multiply_far(layer, 3)
        for part in (0, 1):
            finish(layer, part)
            if layer + 1 < layers:
                for kind in FIRST + SECOND:
                    if kind[1] == part:
                        input_copy(layer + 1, 0, kind).start()
        if layer == 0:
            @pl.when(place.outer)
            def _():
                ship_copy(0).start()
                ship_copy(1).start()
            drain_weights(0)

    @pl.when(place.inner)
    def _():
        ship_copy(0).wait_recv()
        ship_copy(1).wait_recv()
        stage_copy().start()
        stage_copy(True).wait_recv()
        for kind in FIRST + SECOND:
            spread_copy(0, kind).start()
        for kind in FIRST:
            spread_copy(0, kind, True).wait_recv()
        for kind in ONWARD:
            spread_copy(1, kind).start()
        for kind in SECOND:
            spread_copy(0, kind, True).wait_recv()
        for kind in ONWARD:
            spread_copy(1, kind, True).wait_recv()

    planes = place.planes
    bhalf = learner_rows // 2
    bf16, f32 = jnp.bfloat16, jnp.float32
    top = layers - 1
    own_rows = pl.ds(pl.multiple_of(core * learner_rows, learner_rows), learner_rows)
    other_rows = pl.ds(pl.multiple_of((1 - core) * learner_rows, learner_rows), learner_rows)
    slot_width = width // (2 * planes)

    def pair_grads(layer, arriving=False):
        span = pair_grad.at[layer, other_rows if arriving else own_rows]
        return remote(span, span, p_sent.at[1, layer], p_landed.at[1, layer], place.to_core)

    def head_swap(arriving=False):
        return remote(head_pair.at[0], head_pair.at[1], h_sent.at[2], h_landed.at[2],
                      place.to_core)


    def small(stage, peer):
        return remote(head_send.at[stage], head_land.at[stage], h_sent.at[stage],
                      h_landed.at[stage], peer)

    outputs_used = head_raw.shape[0]
    partial_head = lax.dot_general(
        head_weights[...], last_buf[...], (((1,), (1,)), ((), ())), preferred_element_type=f32)
    for stage, peer in enumerate((place.to_x, place.to_y)):
        head_send[stage] = partial_head
        small(stage, peer).start()
        small(stage, peer).wait_recv()
        partial_head = head_send[stage] + head_land[stage]
    head_send[2] = partial_head
    actor_result[...] = head_send[2, pl.ds(0, outputs_used - 1), pl.ds(learner_rows, rows - learner_rows)]
    actor_copy = pltpu.make_async_copy(actor_result, actor_out, out_sem.at[0, PIECES])
    actor_copy.start()
    learner_head = head_send[2, :, :learner_rows]
    gradient = trace_columns(learner_head, packed[...], outputs_used - 1).astype(bf16)
    rows_each = learner_rows // 4
    for part in range(4):
        span = pl.ds(part * rows_each, rows_each)
        column = lax.dot_general(
            gradient[:, part * rows_each:(part + 1) * rows_each], head_weights[...],
            (((0,), (0,)), ((), ())), preferred_element_type=f32)
        value = total[top, span, :]
        sigma = jax.nn.sigmoid(value)
        slope = sigma * (1.0 + value * (1.0 - sigma))
        pair_grad[top, pl.ds(pl.multiple_of(core * learner_rows + part * rows_each, rows_each), rows_each), :] = (
            column * slope).astype(bf16)
    pair_grads(top).start()
    head_pair[0] = lax.dot_general(
        gradient, last_buf[pl.ds(0, learner_rows), :], (((1,), (0,)), ((), ())),
        preferred_element_type=f32)
    head_swap().start()

    lanes = ((place.to_x, place.to_y), (place.to_y, place.to_x))
    near = ((place.near_x, place.near_y), (place.near_y, place.near_x))
    far_quarter = (place.near_x + 2) % 4

    def first_copy(part, slot):
        span = pl.ds(slot * bhalf, bhalf)
        return remote(weight_buf.at[0, part, span], weight_buf.at[0, 2 + part, span], f_sent.at[0, part, slot],
                      f_landed.at[0, part, slot], lanes[part][0])

    def second_copy(part):
        span = pl.ds(part * bhalf, bhalf)
        return remote(weight_buf.at[0, 4, span], weight_buf.at[0, 5, span], f_sent.at[1, part, 0],
                      f_landed.at[1, part, 0], lanes[part][1])

    def input_quarter(quarter, rows_of):
        parts = []
        for block in range(2):
            parts.append(lax.dot_general(
                pair_grad[top, rows_of, :], weight_buf[top, 2 * quarter + block],
                (((1,), (1,)), ((), ())), preferred_element_type=f32))
        return parts

    cores = pl.multiple_of(core * learner_rows, learner_rows)

    def rows_at(part):
        return pl.ds(pl.multiple_of(cores + part * bhalf, bhalf), bhalf)

    def block_cols(block):
        return pl.ds(block * in_block, in_block)

    def send_first(part, slot, quarter):
        for block, value in enumerate(input_quarter(quarter, rows_at(part))):
            weight_buf[0, part, pl.ds(slot * bhalf, bhalf), block_cols(block)] = value.astype(bf16)
        first_copy(part, slot).start()

    def keep_quarter(part, slot, quarter):
        for block, value in enumerate(input_quarter(quarter, rows_at(part))):
            keep[part, slot, :, block_cols(block)] = value

    def order(step):
        table = []
        for at in range(planes):
            up = list(range(planes - 1, at, -1))
            down = list(range(0, at))
            mixed = up + down if len(up) >= len(down) else down + up
            table.append((mixed + [at])[step])
        plane = table[-1]
        for at in range(planes - 1):
            plane = jnp.where(z == at, table[at], plane)
        return plane

    def top_order(step):
        low = (planes - 1, planes // 2, 0)[step]
        high = (0, planes // 2 - 1, planes - 1)[step]
        return jnp.where(z < planes // 2, low, high)

    def line_send(layer, plane, piece, way):
        source = line.at[layer, plane, pl.ds(piece * piece_rows, piece_rows)]
        if way == 0:
            slot = plane
        else:
            slot = jnp.where(plane == z - 1, planes, plane)
        target = line.at[layer, slot, pl.ds(piece * piece_rows, piece_rows)]
        return remote(source, target, lz_sent.at[layer, plane, piece],
                      lz_landed.at[layer, slot, piece], place.to_way[way])

    def line_arrival(layer, slot, piece):
        span = line.at[layer, slot, pl.ds(piece * piece_rows, piece_rows)]
        return remote(span, span, lz_sent.at[layer, 0, piece],
                      lz_landed.at[layer, slot, piece], place.to_core)

    def product(layer, plane, piece, columns):
        contract = (((0,), (0,)), ((), ()))
        mine = pl.ds(pl.multiple_of(core * in_block + piece * piece_rows, piece_rows), piece_rows)
        value = lax.dot_general(
            input_buf[layer, plane, pl.ds(0, learner_rows), mine],
            pair_grad[layer, own_rows, columns], contract, preferred_element_type=f32)
        value = value + lax.dot_general(
            pair_in[layer, plane, :, pl.ds(piece * piece_rows, piece_rows)],
            pair_grad[layer, other_rows, columns], contract, preferred_element_type=f32)
        if layer == top:
            for owner in range(2):
                value = value + lax.dot_general(
                    ship[plane, owner_rows[owner], pl.ds(piece * piece_rows, piece_rows)],
                    weight_buf[0, 6 + owner, :, columns], contract, preferred_element_type=f32)
        return value

    tile = PRODUCT_TILE
    tiles = width // tile

    def over_tiles(body):
        def step(index, carry):
            body(pl.ds(pl.multiple_of(index * tile, tile), tile))
            return carry
        lax.fori_loop(0, tiles, step, 0)

    def pass_on(layer, step):
        if layer == top:
            plane = top_order(step)
            upward = plane > z
            fed = plane == place.mate
        else:
            plane = order(step)
            upward = plane > z
            fed = jnp.where(upward, z > 0, z + 1 < planes)
        for piece in range(PIECES):
            span = pl.ds(piece * piece_rows, piece_rows)

            @pl.when(fed)
            def _():
                line_arrival(layer, plane, piece).wait_recv()

                def body(columns):
                    value = product(layer, plane, piece, columns)
                    value = value + line[layer, plane, span, columns].astype(f32)
                    line[layer, plane, span, columns] = value.astype(bf16)
                over_tiles(body)

            @pl.when(jnp.logical_not(fed))
            def _():
                def body(columns):
                    value = product(layer, plane, piece, columns)
                    line[layer, plane, span, columns] = value.astype(bf16)
                over_tiles(body)

            pl.when(upward)(line_send(layer, plane, piece, 0).start)
            pl.when(jnp.logical_not(upward))(line_send(layer, plane, piece, 1).start)

    def head_line(plane, way, receiving):
        slot = plane
        if way == 1 and not receiving:
            slot = jnp.where(plane == z - 1, planes, plane)
        return remote(head_sum.at[plane], head_sum.at[slot], hl_sent.at[plane],
                      hl_landed.at[slot], place.to_core if receiving else place.to_way[way])

    def head_columns(which, plane):
        start = pl.multiple_of((2 * plane + core) * slot_width, slot_width)
        return head_pair[which, :, pl.ds(start, slot_width)]

    def head_pass(step):
        plane = order(step)
        upward = plane > z
        fed = jnp.where(upward, z > 0, z + 1 < planes)
        own = head_columns(0, plane) + head_columns(1, plane)

        @pl.when(fed)
        def _():
            head_line(plane, 0, True).wait_recv()
            head_sum[plane] = head_sum[plane] + own

        @pl.when(jnp.logical_not(fed))
        def _():
            head_sum[plane] = own

        pl.when(upward)(head_line(plane, 0, False).start)
        pl.when(jnp.logical_not(upward))(head_line(plane, 1, False).start)

    def head_final():
        head_land[0, :, pl.ds(0, slot_width)] = head_columns(0, z) + head_columns(1, z)
        for slot, present in ((z, z > 0), (planes, z + 1 < planes)):
            @pl.when(present)
            def _():
                head_line(slot, 0, True).wait_recv()
                head_land[0, :, pl.ds(0, slot_width)] += head_sum[slot]
        head_result[...] = head_land[0, pl.ds(0, outputs_used), pl.ds(0, slot_width)]
        pltpu.make_async_copy(head_result, head_grads_out, out_sem.at[1, PIECES]).start()

    def drain(layer, step):
        plane = top_order(step) if layer == top else order(step)
        for piece in range(PIECES):
            span = line.at[layer, plane, pl.ds(piece * piece_rows, piece_rows)]
            remote(span, span, lz_sent.at[layer, plane, piece],
                   lz_landed.at[layer, plane, piece], place.to_core).wait_send()

    def own_product(layer):
        for piece in range(PIECES):
            span = pl.ds(piece * piece_rows, piece_rows)

            def body(columns):
                total[layer, span, columns] = product(layer, z, piece, columns)
            over_tiles(body)

    def own_add(layer):
        for piece in range(PIECES):
            span = pl.ds(piece * piece_rows, piece_rows)
            if layer == top:
                cases = ((z, z >= planes // 2), (planes, z < planes // 2))
            else:
                cases = ((z, z > 0), (planes, z + 1 < planes))
            for slot, present in cases:
                @pl.when(present)
                def _():
                    line_arrival(layer, slot, piece).wait_recv()
                    total[layer, span, :] += line[layer, slot, span, :].astype(f32)
            pltpu.make_async_copy(
                total.at[layer, span], grads_out.at[layer, span],
                out_sem.at[layer, piece]).start()


    @pl.when(place.outer)
    def _():
        for piece in range(2):
            grad_ship(piece).start()
    for part in range(2):
        send_first(part, 0, far_quarter)
    for part in range(2):
        send_first(part, 1, near[part][0])
    for part in range(2):
        keep_quarter(part, 1, near[part][1])
        keep_quarter(part, 0, group)
    head_swap(True).wait_recv()
    head_pass(0)
    pair_grads(top, True).wait_recv()
    pair_inputs(top).wait_recv()
    for part in range(2):
        first_copy(part, 0).wait_recv()
        weight_buf[0, 4, pl.ds(part * bhalf, bhalf), :] = (
            keep[part, 1] + weight_buf[0, 2 + part, pl.ds(0, bhalf), :].astype(f32)).astype(bf16)
        second_copy(part).start()

    @pl.when(place.inner)
    def _():
        for piece in range(2):
            grad_ship(piece).wait_recv()
            grad_swap(piece).start()
        for piece in range(2):
            grad_swap(piece, True).wait_recv()
        pass_on(top, 0)
    for part in range(2):
        first_copy(part, 1).wait_recv()
        second_copy(part).wait_recv()
        summed = keep[part, 0] + weight_buf[0, 2 + part, pl.ds(bhalf, bhalf), :].astype(f32)
        summed = summed + weight_buf[0, 5, pl.ds(part * bhalf, bhalf), :].astype(f32)
        value = total[0, pl.ds(part * bhalf, bhalf), :]
        sigma = jax.nn.sigmoid(value)
        slope = sigma * (1.0 + value * (1.0 - sigma))
        pair_grad[0, rows_at(part), :] = (summed * slope).astype(bf16)
    pair_grads(0).start()
    pl.when(place.inner)(functools.partial(pass_on, top, 1))
    pair_grads(0, True).wait_recv()
    pair_inputs(0).wait_recv()
    pass_on(0, 0)
    pl.when(place.inner)(functools.partial(pass_on, top, 2))
    head_pass(1)
    head_pass(2)
    pass_on(0, 1)
    pl.when(place.inner)(functools.partial(own_product, top))

    @pl.when(place.outer)
    def _():
        total[top, pl.ds(0, learner_rows), :] = jnp.zeros((learner_rows, width), f32)
    pass_on(0, 2)
    own_product(0)
    own_add(top)
    head_final()
    own_add(0)

    for layer in range(layers):
        pair_inputs(layer).wait_send()
        pair_grads(layer).wait_send()
        for step in range(planes - 1):
            if layer == top:
                pl.when(place.inner)(functools.partial(drain, layer, step))
            else:
                drain(layer, step)
        for piece in range(PIECES):
            span = pl.ds(piece * piece_rows, piece_rows)
            pltpu.make_async_copy(
                total.at[layer, span], grads_out.at[layer, span],
                out_sem.at[layer, piece]).wait()
    for part in range(2):
        for slot in range(2):
            first_copy(part, slot).wait_send()
        second_copy(part).wait_send()
    small(0, place.to_x).wait_send()
    small(1, place.to_y).wait_send()
    head_swap().wait_send()
    for step in range(planes - 1):
        head_line(order(step), 0, True).wait_send()
    actor_copy.wait()
    pltpu.make_async_copy(head_result, head_grads_out, out_sem.at[1, PIECES]).wait()

    for layer in range(layers):
        for kind in FIRST + SECOND:
            input_copy(layer, 0, kind).wait_send()
        for kind in ONWARD:
            input_copy(layer, 1, kind).wait_send()
    for layer in range(1, layers):
        drain_weights(layer)

    @pl.when(place.outer)
    def _():
        for other in range(2):
            ship_copy(other).wait_send()
            grad_ship(other).wait_send()

    @pl.when(place.inner)
    def _():
        stage_copy().wait_send()
        for kind in FIRST + SECOND:
            spread_copy(0, kind).wait_send()
        for kind in ONWARD:
            spread_copy(1, kind).wait_send()
        for piece in range(2):
            grad_swap(piece).wait_send()


def trace_columns(outputs, packed, actions_total):
    count, columns = outputs.shape
    row = lax.broadcasted_iota(jnp.int32, (count, columns), 0)
    is_action = row < actions_total
    behave, action = packed[0:1], packed[1:2]
    rewards, finished, live = packed[2:3], packed[3:4], packed[4:5]

    def after(value, reach):
        return pltpu.roll(value, columns - reach, 1)

    peak = jnp.max(jnp.where(is_action, outputs, -jnp.inf), axis=0, keepdims=True)
    shifted = jnp.where(is_action, outputs - peak, 0.0)
    weight = jnp.where(is_action, jnp.exp(shifted), 0.0)
    scale = jnp.sum(weight, axis=0, keepdims=True)
    log_policy = jnp.where(is_action, shifted - jnp.log(scale), 0.0)
    probability = jnp.where(is_action, jnp.exp(log_policy), 0.0)
    chosen = jnp.where(row == action.astype(jnp.int32), 1.0, 0.0)
    ratio = jnp.exp(jnp.sum(log_policy * chosen, axis=0, keepdims=True) - behave)
    clipped = jnp.minimum(ratio, 1.0)
    discount = discount_rate * (1.0 - finished)
    current = jnp.sum(jnp.where(row == actions_total, outputs, 0.0), axis=0, keepdims=True)
    corrections = live * clipped * (rewards + discount * after(current, 1) - current)
    factors = live * discount * clipped
    reach = 1
    while reach < columns:
        corrections = corrections + factors * after(corrections, reach)
        factors = factors * after(factors, reach)
        reach *= 2
    targets = current + corrections
    advantage = clipped * (rewards + discount * after(targets, 1) - current)
    entropy = -jnp.sum(probability * log_policy, axis=0, keepdims=True)
    logit_grad = (
        -advantage * (chosen - probability)
        + entropy_weight * probability * (log_policy + entropy)
    ) / loss_divisor
    value_grad = -value_weight * (targets - current) / loss_divisor
    result = jnp.where(is_action, logit_grad, jnp.where(row == actions_total, value_grad, 0.0))
    return jnp.where(live > 0.0, result, 0.0)


def exact_dot(left, right, dims):
    return lax.dot_general(
        left, right, (dims, ((), ())), precision=lax.Precision.HIGHEST,
        preferred_element_type=jnp.float32)


def prepare(head_own, acting_own, actions_own, rewards_own, finished_own, head_weights, packed):
    padded, used = head_weights.shape[0], head_own.shape[0]
    row = lax.broadcasted_iota(jnp.int32, (padded, used), 0)
    column = lax.broadcasted_iota(jnp.int32, (padded, used), 1)
    select = jnp.where(row == column, 1.0, 0.0).astype(jnp.bfloat16)
    head_weights[...] = lax.dot_general(
        select, head_own[...], (((1,), (0,)), ((), ())), preferred_element_type=jnp.float32
    ).astype(jnp.bfloat16)
    actions_total, trajectories, steps = acting_own.shape
    columns = packed.shape[1]
    span = columns // trajectories
    step = lax.broadcasted_iota(jnp.int32, (steps, columns), 0)
    place = lax.broadcasted_iota(jnp.int32, (steps, columns), 1)
    spread = jnp.where(place % span == step, 1.0, 0.0)
    owner = lax.broadcasted_iota(jnp.int32, (trajectories, columns), 0)
    where = lax.broadcasted_iota(jnp.int32, (trajectories, columns), 1)
    mine = where // span == owner

    def flat(array):
        wide = exact_dot(array.astype(jnp.float32), spread, ((1,), (0,)))
        return jnp.sum(jnp.where(mine, wide, 0.0), axis=0, keepdims=True)

    action = flat(actions_own[...])
    scores = jnp.concatenate([flat(acting_own[at]) for at in range(actions_total)], axis=0)
    peak = jnp.max(scores, axis=0, keepdims=True)
    shifted = scores - peak
    scale = jnp.sum(jnp.exp(shifted), axis=0, keepdims=True)
    kind = lax.broadcasted_iota(jnp.int32, (actions_total, columns), 0)
    taken = jnp.sum(jnp.where(kind == action.astype(jnp.int32), shifted, 0.0), axis=0, keepdims=True)
    packed[0:1, :] = taken - jnp.log(scale)
    packed[1:2, :] = action
    packed[2:3, :] = flat(rewards_own[...])
    packed[3:4, :] = flat(finished_own[...])
    live = lax.broadcasted_iota(jnp.int32, (1, columns), 1) % span < steps
    packed[4:5, :] = jnp.where(live, 1.0, 0.0)


def whole_step(observations, next_observations, weights, head_weights, acting, *per_step):
    layers, in_block, width = weights.shape
    learner_rows = observations.shape[0]
    rows = learner_rows + next_observations.shape[0]
    used = head_weights.shape[0]
    padded = -(-used // 16) * 16
    planes = lax.axis_size("dp") // 2
    bf16, f32 = jnp.bfloat16, jnp.float32
    half = learner_rows // 2
    dma = pltpu.SemaphoreType.DMA
    hbm = pl.BlockSpec(memory_space=pltpu.HBM)
    slot_width = width // (2 * planes)
    return pl.pallas_call(
        step_kernel,
        out_shape=(
            jax.ShapeDtypeStruct((layers, in_block, width), f32),
            jax.ShapeDtypeStruct((used, slot_width), f32),
            jax.ShapeDtypeStruct((used - 1, rows - learner_rows), f32),
        ),
        in_specs=[hbm] * 8,
        out_specs=(hbm,) * 3,
        scratch_shapes=[
            pltpu.VMEM((layers, 2 * planes, in_block, width), bf16),
            pltpu.VMEM((layers, 4, rows, width), bf16),
            pltpu.VMEM((rows, width), bf16),
            pltpu.VMEM((layers, rows, width), f32),
            pltpu.VMEM((layers, 4, learner_rows, in_block), bf16),
            pltpu.VMEM((layers, 2 * learner_rows, width), bf16),
            pltpu.VMEM((layers, planes + 1, in_block, width), bf16),
            pltpu.VMEM((2, 2, half, width), f32),
            pltpu.VMEM((4, 2 * learner_rows, in_block), bf16),
            pltpu.VMEM((learner_rows, in_block), bf16),
            pltpu.VMEM((3, padded, rows), f32),
            pltpu.VMEM((2, padded, rows), f32),
            pltpu.VMEM((2, padded, width), f32),
            pltpu.VMEM((planes + 1, padded, slot_width), f32),
            pltpu.VMEM(head_weights.shape, bf16),
            pltpu.VMEM(acting.shape, f32),
        ] + [pltpu.VMEM(array.shape, array.dtype) for array in per_step] + [
            pltpu.VMEM((padded, width), bf16),
            pltpu.VMEM((8, learner_rows), f32),
            pltpu.VMEM((used, slot_width), f32),
            pltpu.VMEM((used - 1, rows - learner_rows), f32),
            dma((7 + layers,)),
            dma((layers, 2, 2, 2)), dma((layers, 2, 2, 2)),
            dma((layers, 2, 4, PIECES)), dma((layers, 2, 4, PIECES)),
            dma((layers, 2, 4, PIECES)), dma((layers, 2, 4, PIECES)),
            dma((2, layers)), dma((2, layers)),
            dma((layers, planes + 1, PIECES)), dma((layers, planes + 1, PIECES)),
            dma((2, 2, 2)), dma((2, 2, 2)),
            dma((3,)), dma((3,)),
            dma((planes + 1,)), dma((planes + 1,)),
            dma((16,)), dma((16,)),
            dma((layers, PIECES + 1)),
        ],
        compiler_params=pltpu.CompilerParams(
            collective_id=0, has_side_effects=True, vmem_limit_bytes=VMEM_LIMIT),
        name="learner_step",
    )(observations, next_observations, weights, head_weights, acting, *per_step)


def per_device_line(
    observations, next_observations, trunk_weights, head_weights,
    acting_policy_logits, actions, rewards, episode_finished,
):
    traj_count, step_count, feature_block = observations.shape
    learner_rows = traj_count * step_count
    trunk_grads, head_grads, actor_logits = whole_step(
        observations.reshape(learner_rows, feature_block), next_observations, trunk_weights,
        head_weights.T, acting_policy_logits.transpose(2, 0, 1), actions, rewards,
        episode_finished)
    return trunk_grads, head_grads.T, actor_logits.T


def solution(mesh):
    in_specs = (
        P("dp", None, "group"),
        P("dp", "group"),
        P(None, "dp", "group"),
        P("group", None),
        P("dp", None, None),
        P("dp", None),
        P("dp", None),
        P("dp", None),
    )
    out_specs = (P(None, "dp", "group"), P(("group", "dp"), None), P("dp", None))
    body = functools.partial(per_device, mesh.shape["group"], mesh.shape["dp"])
    if (mesh.shape["group"], mesh.shape["dp"]) == (4, 8):
        body = per_device_line
    return jax.shard_map(
        body, mesh=mesh, in_specs=in_specs, out_specs=out_specs, check_vma=False
    )
```
